256 devices in a mesh: gx: 16 (over z_lo, x), gy: 4 (over y), gz: 4 (over z_hi, core).
Axes of the slice: x: 4, y: 4, z: 8 (z_hi: 2, z_lo: 4; z = z_hi * 4 + z_lo), core: 2. Of those that a mesh axis runs over, the one named last changes fastest.
Arguments:
- tokens: bfloat16 [8192, 4608], P('gx', 'gy'), may hold values from -6 to 6
- base_up_weight: bfloat16 [4608, 18432], P('gy', ('gz', 'gx')), may hold values from -0.09375 to 0.09375
- adapter_down_weight: bfloat16 [64, 16, 4608], P(None, None, 'gy'), may hold values from -0.09375 to 0.09375
- adapter_up_weight: bfloat16 [64, 16, 18432], P('gx', None, 'gz'), may hold values from -1.5 to 1.5
- block_adapter_index: int32 [64], P('gx'), may hold values from 0 to 63
- request_rows: int32 [64], P('gx'), may hold values from 1 to 128
Outputs:
- projected: bfloat16 [8192, 18432], P(('gx', 'gy'), 'gz')
The draws below stay inside these ranges and needn't reach their ends.
Inputs may be any that keep to these rules, and one draw needn't show every extreme that they name: `request_rows`: live rows of each block.
All inputs are finite; a program needn't handle non-finite values.
Results may differ from the reference program's by a relative error of at most 0.0047.
Values may be sent and summed in bfloat16 or wider, within the bound.
A program may use at most 128 MiB of HBM per device.

```python
import jax
import jax.numpy as jnp
from jax import lax

MODEL_WIDTH = 4608
HIDDEN_UNITS = 18432
ADAPTER_RANK = 16
ADAPTER_COUNT = 64
BLOCK = 128
BLOCKS = 64
ROWS = 8192


def touch_ends(array, rng, low, largest):
    place = [jax.random.randint(jax.random.fold_in(rng, axis), (), 0, length) for axis, length in enumerate(array.shape)]
    main_axis = array.shape.index(max(array.shape))
    beside = place[:main_axis] + [(place[main_axis] + 1) % array.shape[main_axis]] + place[main_axis + 1:]
    return array.at[tuple(place)].set(low).at[tuple(beside)].set(largest)


def block_scale(own_key, shape, pieces, least, high):
    factor_of = 1.0
    for axis_at, parts in pieces:
        steps = jax.random.uniform(jax.random.fold_in(jax.random.fold_in(own_key, 6), axis_at), (parts,), jnp.float32, least / len(pieces), high / len(pieces))
        factor_of = factor_of * jnp.repeat(jnp.exp(steps), shape[axis_at] // parts).reshape((-1,) + (1,) * (len(shape) - 1 - axis_at))
    return factor_of


def gaussian(key, dims, scale, most, shards=(), kind=jnp.bfloat16):
    values = scale * jax.random.normal(key, dims, jnp.float32)
    if shards:
        values = values * block_scale(key, dims, shards, -0.22, 0.18)
    return jnp.clip(values, -most, most).astype(kind)


def setup_inputs(seed: int = 0) -> dict:
    streams_of = jax.random.split(jax.random.key(seed), 7)
    return {
        "tokens": gaussian(streams_of[0], (ROWS, MODEL_WIDTH), 1.0, 6.0, ((0, 16), (1, 4))),
        "base_up_weight": gaussian(streams_of[1], (MODEL_WIDTH, HIDDEN_UNITS), MODEL_WIDTH ** -0.5, 0.09375, ((0, 4), (1, 64))),
        "adapter_down_weight": gaussian(streams_of[2], (ADAPTER_COUNT, ADAPTER_RANK, MODEL_WIDTH), MODEL_WIDTH ** -0.5, 0.09375, ((2, 4),)),
        "adapter_up_weight": gaussian(streams_of[3], (ADAPTER_COUNT, ADAPTER_RANK, HIDDEN_UNITS), ADAPTER_RANK ** -0.5, 1.5, ((0, 16), (2, 4))),
        "block_adapter_index": touch_ends(jax.random.randint(streams_of[4], (BLOCKS,), 0, ADAPTER_COUNT), jax.random.fold_in(streams_of[4], 1), 0, ADAPTER_COUNT - 1).astype(jnp.int32),
        "request_rows": touch_ends(jax.random.randint(streams_of[5], (BLOCKS,), 1, BLOCK + 1), jax.random.fold_in(streams_of[5], 1), 1, BLOCK).astype(jnp.int32),
    }


def reference(tokens, base_up_weight, adapter_down_weight, adapter_up_weight, block_adapter_index, request_rows):
    blocks = block_adapter_index.shape[0]
    tok_blocks = tokens.reshape(blocks, BLOCK, MODEL_WIDTH)

    def one_block(items):
        block_tokens, adapter_index, live_count = items
        down_factor = lax.dynamic_index_in_dim(adapter_down_weight, adapter_index, 0, keepdims=False)
        up_factor = lax.dynamic_index_in_dim(adapter_up_weight, adapter_index, 0, keepdims=False)
        shrink = jnp.dot(block_tokens, down_factor.T, preferred_element_type=jnp.float32)
        shrink_low = shrink.astype(jnp.bfloat16)
        expand = jnp.dot(shrink_low, up_factor, preferred_element_type=jnp.float32)
        base = jnp.dot(block_tokens, base_up_weight, preferred_element_type=jnp.float32)
        live_mask = jnp.arange(BLOCK, dtype=jnp.int32) < live_count
        return jnp.where(live_mask[:, None], base + 2.0 * expand, 0.0).astype(jnp.bfloat16)

    result = lax.map(one_block, (tok_blocks, block_adapter_index, request_rows))
    return result.reshape(blocks * BLOCK, HIDDEN_UNITS)
```

```python
import functools

import jax
import jax.numpy as jnp
from jax import lax
from jax.experimental import pallas as pl
from jax.experimental.pallas import tpu as pltpu
from jax.sharding import PartitionSpec as P

BLOCK = 128
RANK = 16
CATALOG = 64
WIDTH = 1152
COLS = 288
HALF = COLS // 2
SLICE = 4 * COLS
UNITS = 16
LAG_RELAY = 2
LAG_SUM = 4
BF = jnp.bfloat16
F32 = jnp.float32
LAST = (((1,), (1,)), ((), ()))


def swap23(n):
    return n + n // 2 - 2 * (n // 3)


def unit_of(step):
    turn = (step + 3) // 4 % 4
    extra = 1 - (turn + 3) // 4
    return swap23(turn), swap23(((step + 3) % 4 + extra) % 4)


def kernel(
    idx_ref, live_ref, tok_hbm, wt_hbm, down_hbm, up_hbm, out_ref,
    toks, wts, down, up, parts, relay, arrived, sums, final,
    idx_all, idx_s, spread, picked, zpicks, chosen, upfin, shr, shr_in,
    local_sem, tok_s, tok_r, tokf_s, tokp_s, tokp_r, w_s, w_r, wf_s,
    r1_s, r1_r, r2_s, r2_r, fin_s, fin_r,
    ixa_s, ixa_r, ixb_s, ixb_r, u1_s, u1_r, u2_s, u2_r, u3_s, u3_r, sh_s, sh_r,
):
    gx = lax.axis_index("gx")
    y = lax.axis_index("gy")
    gz = lax.axis_index("gz")
    z, x = gx // 4, gx % 4
    zh, core = gz // 2, gz % 2
    ring = zh * 4 + z

    def along_x(step):
        return (z * 4 + (x + step) % 4, y, gz)

    def along_y(step):
        return (gx, (y + step) % 4, gz)

    def along_z(step):
        return (((z + step) % 4) * 4 + x, y, gz)

    def on_ring(step):
        place = (ring + step) % 8
        return ((place % 4) * 4 + x, y, (place // 4) * 2 + core)

    partner = (gx, y, zh * 2 + 1 - core)

    def remote(src, dst, send, recv, to):
        return pltpu.make_async_remote_copy(
            src_ref=src, dst_ref=dst, send_sem=send, recv_sem=recv,
            device_id=to, device_id_type=pl.DeviceIdType.MESH,
        )

    first, second = 2 * core, 2 * core + 1

    def tok_own(way, part):
        block = first if part == 0 else second
        return remote(
            tok_hbm.at[block], toks.at[3 if way > 0 else 1, block],
            tok_s.at[0 if way > 0 else 1, part], tok_r.at[2 if way > 0 else 0, part], on_ring(way),
        )

    def tok_forward(way):
        block = first if way > 0 else second
        part = 0 if way > 0 else 1
        return remote(
            toks.at[3 if way > 0 else 1, block], toks.at[2, block],
            tokf_s.at[part], tok_r.at[1, part], on_ring(way),
        )

    def tok_partner(slot, part):
        block = first if part == 0 else second
        return remote(
            toks.at[slot, block], toks.at[slot, block],
            tokp_s.at[slot - 1, part], tokp_r.at[slot - 1, part], partner,
        )

    def tok_arrival(slot, part):
        block = first if part == 0 else second
        return remote(
            toks.at[slot, block], toks.at[slot, block],
            tokp_s.at[slot - 1, part], tok_r.at[slot - 1, part], partner,
        )

    def tok_partner_arrival(slot, part):
        block = 2 * (1 - core) + part
        return remote(
            toks.at[slot, block], toks.at[slot, block],
            tokp_s.at[slot - 1, part], tokp_r.at[slot - 1, part], partner,
        )

    def w_own(way, part):
        return remote(
            wt_hbm.at[part], wts.at[3 if way > 0 else 1, part],
            w_s.at[0 if way > 0 else 1, part], w_r.at[2 if way > 0 else 0, part], along_x(way % 4),
        )

    def w_forward(way):
        part = 0 if way > 0 else 1
        return remote(
            wts.at[3 if way > 0 else 1, part], wts.at[2, part],
            wf_s.at[part], w_r.at[1, part], along_x(way % 4),
        )

    def w_arrival(slot, part):
        return remote(
            wts.at[slot, part], wts.at[slot, part],
            wf_s.at[part], w_r.at[slot - 1, part], along_x(1),
        )

    def relay_copy(step, part):
        return remote(
            parts.at[step, (y + 2) % 4, part], relay.at[step, part],
            r1_s.at[step, part], r1_r.at[step, part], along_y(1 if part == 0 else 3),
        )

    def sum_copy(step, part):
        way = 1 if part == 0 else 3
        return remote(
            parts.at[step, (y + way) % 4], arrived.at[step, part],
            r2_s.at[step, part], r2_r.at[step, part], along_y(way),
        )

    def final_copy(step):
        s, t = unit_of(step)
        chunk = (x + t) % 4
        return remote(
            sums.at[step], final.at[z, chunk], fin_s.at[step], fin_r.at[z, chunk], along_z(s)
        )

    def index_x(step):
        return remote(
            idx_all.at[z, x], idx_all.at[z, x], ixa_s.at[step - 1], ixa_r.at[step - 1], along_x(step)
        )

    def index_x_arrival(step):
        place = (x + 4 - step) % 4
        return remote(
            idx_all.at[z, place], idx_all.at[z, place],
            ixa_s.at[step - 1], ixa_r.at[step - 1], along_x(step),
        )

    def index_z(step):
        return remote(
            idx_all.at[z], idx_all.at[z], ixb_s.at[step - 1], ixb_r.at[step - 1], along_z(step)
        )

    def index_z_arrival(step):
        place = (z + 4 - step) % 4
        return remote(
            idx_all.at[place], idx_all.at[place],
            ixb_s.at[step - 1], ixb_r.at[step - 1], along_z(step),
        )

    def up_spread(step):
        columns = pl.ds(pl.multiple_of((x + step) % 4 * SLICE, SLICE), SLICE)
        return remote(
            up.at[:, :, columns], spread.at[x], u1_s.at[step - 1], u1_r.at[step - 1], along_x(step)
        )

    def up_spread_arrival(step):
        place = (x + 4 - step) % 4
        return remote(
            spread.at[place], spread.at[place], u1_s.at[step - 1], u1_r.at[step - 1], along_x(step)
        )

    def up_pick(step):
        return remote(
            picked.at[(z + step) % 4], zpicks.at[step - 1],
            u2_s.at[step - 1], u2_r.at[step - 1], along_z(step),
        )

    def up_last(step):
        return remote(
            chosen.at[(x + step) % 4], upfin.at[x], u3_s.at[step - 1], u3_r.at[step - 1], along_x(step)
        )

    def up_last_arrival(step):
        place = (x + 4 - step) % 4
        return remote(
            upfin.at[place], upfin.at[place], u3_s.at[step - 1], u3_r.at[step - 1], along_x(step)
        )

    def shrink_copy(step):
        return remote(
            shr.at[(y + step) % 4], shr_in.at[step - 1],
            sh_s.at[step - 1], sh_r.at[step - 1], along_y(step),
        )

    loads = [
        pltpu.make_async_copy(tok_hbm, toks.at[0], local_sem.at[0]),
        pltpu.make_async_copy(wt_hbm, wts.at[0], local_sem.at[1]),
        pltpu.make_async_copy(down_hbm, down, local_sem.at[2]),
        pltpu.make_async_copy(up_hbm, up, local_sem.at[3]),
    ]
    for load in loads:
        load.start()

    lane = lax.broadcasted_iota(jnp.int32, (1, 128), 1)
    row = jnp.zeros((1, 128), jnp.int32)
    for block in range(4):
        row = jnp.where(lane == block, idx_ref[block], row)
    idx_all[z, x] = row

    barrier = pltpu.get_barrier_semaphore()
    peers = [along_x(n) for n in (1, 2, 3)] + [along_y(n) for n in (1, 2, 3)]
    peers += [along_z(n) for n in (1, 2, 3)] + [on_ring(1), on_ring(-1), partner]
    for peer in peers:
        pl.semaphore_signal(barrier, inc=1, device_id=peer, device_id_type=pl.DeviceIdType.MESH)
    pl.semaphore_wait(barrier, len(peers))

    for n in (1, 2, 3):
        index_x(n).start()
    for way, order in ((1, (0, 1)), (-1, (1, 0))):
        for part in order:
            w_own(way, part).start()
            tok_own(way, part).start()

    for load in loads:
        load.wait()
    for block in range(4):
        chosen_down = down[idx_ref[block]]
        shr[block] = lax.dot_general(chosen_down, toks[0, block], LAST, preferred_element_type=F32)
    for n in (1, 2, 3):
        index_x_arrival(n).wait_recv()
    for n in (1, 2, 3):
        index_z(n).start()
        shrink_copy(n).start()

    def step_body(step, carry):
        @pl.when(step == 1)
        def _():
            tok_arrival(1, 1).wait_recv()
            tok_forward(-1).start()
            tok_partner(1, 1).start()
            tok_arrival(3, 0).wait_recv()
            tok_forward(1).start()
            tok_partner(3, 0).start()
            w_arrival(3, 0).wait_recv()
            w_forward(1).start()
            w_arrival(1, 1).wait_recv()
            w_forward(-1).start()
            for n in (1, 3, 2):
                up_spread(n).start()
            tok_arrival(1, 0).wait_recv()
            tok_partner(1, 0).start()
            tok_partner_arrival(1, 1).wait_recv()
            tok_partner_arrival(1, 0).wait_recv()

        @pl.when(step == 2)
        def _():
            tok_arrival(3, 1).wait_recv()
            tok_partner(3, 1).start()
            w_arrival(1, 0).wait_recv()

        @pl.when(step == 3)
        def _():
            w_arrival(3, 1).wait_recv()

        @pl.when(step == 4)
        def _():
            w_arrival(2, 0).wait_recv()
            w_arrival(2, 1).wait_recv()

        @pl.when(step == 5)
        def _():
            tok_partner_arrival(3, 0).wait_recv()
            tok_partner_arrival(3, 1).wait_recv()

        @pl.when(step == 6)
        def _():
            for part in (0, 1):
                tok_arrival(2, part).wait_recv()
                tok_partner(2, part).start()

        @pl.when(step == 9)
        def _():
            for part in (0, 1):
                tok_partner_arrival(2, part).wait_recv()

        @pl.when(step < UNITS)
        def _():
            s, t = unit_of(step)
            result = lax.dot_general(
                wts[t].reshape(COLS, WIDTH), toks[s].reshape(4 * BLOCK, WIDTH), LAST,
                preferred_element_type=F32,
            ).astype(BF)
            for block in range(4):
                tile = result[:, block * BLOCK : (block + 1) * BLOCK]
                parts[step, block] = tile.reshape(2, HALF, BLOCK)

        @pl.when((step >= LAG_RELAY) & (step < UNITS + LAG_RELAY))
        def _():
            done = step - LAG_RELAY
            for part in (0, 1):
                to = (y + (1 if part == 0 else 3)) % 4
                relay_copy(done, part).wait_recv()
                added = parts[done, to, part].astype(F32) + relay[done, part].astype(F32)
                parts[done, to, part] = added.astype(BF)

        @pl.when(step < UNITS)
        def _():
            for part in (0, 1):
                relay_copy(step, part).start()

        @pl.when((step >= LAG_RELAY) & (step < UNITS + LAG_RELAY))
        def _():
            for part in (0, 1):
                sum_copy(step - LAG_RELAY, part).start()

        @pl.when(step >= LAG_SUM)
        def _():
            done = step - LAG_SUM
            s, t = unit_of(done)
            for part in (0, 1):
                sum_copy(done, part).wait_recv()
            total = parts[done, y].astype(F32) + arrived[done, 0].astype(F32)
            total = (total + arrived[done, 1].astype(F32)).astype(BF)

            @pl.when(s == 0)
            def _():
                final[z, (x + t) % 4] = total

            @pl.when(s > 0)
            def _():
                sums[done] = total
                final_copy(done).start()

        @pl.when(step == 7)
        def _():
            for n in (1, 2, 3):
                index_z_arrival(n).wait_recv()
            to_scalars = pltpu.make_async_copy(idx_all, idx_s, local_sem.at[0])
            to_scalars.start()
            own = pltpu.make_async_copy(
                up.at[:, :, pl.ds(pl.multiple_of(x * SLICE, SLICE), SLICE)], spread.at[x], local_sem.at[1]
            )
            own.start()
            for n in (1, 2, 3):
                up_spread_arrival(n).wait_recv()
            to_scalars.wait()
            own.wait()
            for to_z in range(4):
                for to_x in range(4):
                    local = idx_s[to_z, to_x, 0, y] - 16 * z
                    owned = jnp.where((local >= 0) & (local < 16), 1.0, 0.0).astype(F32)
                    kept = jnp.clip(local, 0, 15)
                    factor = spread[kept // 4, kept % 4].astype(F32) * owned
                    picked[to_z, to_x] = factor.astype(BF)
            for n in (1, 2, 3):
                up_pick(n).start()

        @pl.when(step == 12)
        def _():
            for n in (1, 2, 3):
                up_pick(n).wait_recv()
            for to_x in range(4):
                chosen[to_x] = (picked[z, to_x] + zpicks[0, to_x]) + (zpicks[1, to_x] + zpicks[2, to_x])
            for n in (1, 2, 3):
                up_last(n).start()
            upfin[x] = chosen[x]

        return carry

    lax.fori_loop(0, UNITS + LAG_SUM, step_body, 0)

    for n in (1, 2, 3):
        shrink_copy(n).wait_recv()
    low = (shr[y] + shr_in[0] + (shr_in[1] + shr_in[2])).astype(BF)
    same = lax.broadcasted_iota(jnp.int32, (BLOCK, BLOCK), 0) == lax.broadcasted_iota(
        jnp.int32, (BLOCK, BLOCK), 1
    )
    eye = jnp.where(same, 1.0, 0.0).astype(BF)
    turned = lax.dot_general(eye, low, LAST, preferred_element_type=F32)
    doubled = (2.0 * turned).astype(BF)
    rows = lax.broadcasted_iota(jnp.int32, (BLOCK, 1), 0)
    live = rows < live_ref[y]

    for n in (1, 2, 3):
        up_last_arrival(n).wait_recv()
        for t in range(4):
            place = (z + n) % 4
            remote(
                sums.at[0], final.at[place, t], fin_s.at[0], fin_r.at[place, t], along_z(n)
            ).wait_recv()
    for part in range(4):
        base = lax.dot_general(
            eye, final[part].reshape(SLICE, BLOCK), LAST, preferred_element_type=F32
        )
        extra = jnp.dot(doubled, upfin[part], preferred_element_type=F32)
        out_ref[:, part * SLICE : (part + 1) * SLICE] = jnp.where(live, base + extra, 0.0).astype(BF)

    for n in (1, 2, 3):
        index_x(n).wait_send()
        index_z(n).wait_send()
        up_spread(n).wait_send()
        up_pick(n).wait_send()
        up_last(n).wait_send()
        shrink_copy(n).wait_send()
    for way in (1, -1):
        for part in (0, 1):
            w_own(way, part).wait_send()
            tok_own(way, part).wait_send()
        w_forward(way).wait_send()
        tok_forward(way).wait_send()
    for slot in (1, 2, 3):
        for part in (0, 1):
            tok_partner(slot, part).wait_send()

    def drain(step, carry):
        for part in (0, 1):
            relay_copy(step, part).wait_send()
            sum_copy(step, part).wait_send()

        @pl.when(unit_of(step)[0] > 0)
        def _():
            final_copy(step).wait_send()

        return carry

    lax.fori_loop(0, UNITS, drain, 0)


def body(tokens, base_up_weight, adapter_down_weight, adapter_up_weight, block_adapter_index, request_rows):
    dma = pltpu.SemaphoreType.DMA
    half_tile = (2, HALF, BLOCK)
    any_space = pl.BlockSpec(memory_space=pl.ANY)
    scalars = pl.BlockSpec(memory_space=pltpu.SMEM)
    return pl.pallas_call(
        kernel,
        out_shape=jax.ShapeDtypeStruct((BLOCK, 4 * SLICE), BF),
        in_specs=[scalars, scalars, any_space, any_space, any_space, any_space],
        out_specs=pl.BlockSpec(memory_space=pltpu.VMEM),
        scratch_shapes=[
            pltpu.VMEM((4, 4, BLOCK, WIDTH), BF),
            pltpu.VMEM((4, 2, HALF, WIDTH), BF),
            pltpu.VMEM((CATALOG, RANK, WIDTH), BF),
            pltpu.VMEM((4, RANK, 4 * SLICE), BF),
            pltpu.VMEM((UNITS, 4, *half_tile), BF),
            pltpu.VMEM((UNITS, *half_tile), BF),
            pltpu.VMEM((UNITS, 2, *half_tile), BF),
            pltpu.VMEM((UNITS, *half_tile), BF),
            pltpu.VMEM((4, 4, *half_tile), BF),
            pltpu.VMEM((4, 4, 1, 128), jnp.int32),
            pltpu.SMEM((4, 4, 1, 128), jnp.int32),
            pltpu.VMEM((4, 4, RANK, SLICE), BF),
            pltpu.VMEM((4, 4, RANK, SLICE), BF),
            pltpu.VMEM((3, 4, RANK, SLICE), BF),
            pltpu.VMEM((4, RANK, SLICE), BF),
            pltpu.VMEM((4, RANK, SLICE), BF),
            pltpu.VMEM((4, RANK, BLOCK), F32),
            pltpu.VMEM((3, RANK, BLOCK), F32),
            dma((4,)),
            dma((2, 2)), dma((3, 2)), dma((2,)), dma((3, 2)), dma((3, 2)),
            dma((2, 2)), dma((3, 2)), dma((2,)),
            dma((UNITS, 2)), dma((UNITS, 2)), dma((UNITS, 2)), dma((UNITS, 2)),
            dma((UNITS,)), dma((4, 4)),
            dma((3,)), dma((3,)), dma((3,)), dma((3,)),
            dma((3,)), dma((3,)), dma((3,)), dma((3,)), dma((3,)), dma((3,)),
            dma((3,)), dma((3,)),
        ],
        compiler_params=pltpu.CompilerParams(
            collective_id=0, has_side_effects=True, vmem_limit_bytes=50 * 1024 * 1024
        ),
    )(
        block_adapter_index,
        request_rows,
        tokens.reshape(4, BLOCK, WIDTH),
        base_up_weight.T.reshape(2, HALF, WIDTH),
        adapter_down_weight,
        adapter_up_weight,
    )


def solution(mesh):
    in_specs = (
        P("gx", "gy"),
        P("gy", ("gz", "gx")),
        P(None, None, "gy"),
        P("gx", None, "gz"),
        P("gx"),
        P("gx"),
    )
    out_specs = P(("gx", "gy"), "gz")
    return jax.shard_map(body, mesh=mesh, in_specs=in_specs, out_specs=out_specs, check_vma=False)
```

```python
import functools

import jax
import jax.numpy as jnp
from jax import lax
from jax.experimental import pallas as pl
from jax.experimental.pallas import tpu as pltpu
from jax.sharding import PartitionSpec as P

BLOCK = 128
RANK = 16
CATALOG = 64
WIDTH = 1152
COLS = 288
HALF = COLS // 2
SLICE = 4 * COLS
UNITS = 16
LAG_RELAY = 2
LAG_SUM = 4
PICK_STEP = 8
PAIR_STEP = 11
FAR_STEP = 16
BF = jnp.bfloat16
F32 = jnp.float32
LAST = (((1,), (1,)), ((), ()))


ORDER = (
    (0, 0), (1, 0), (1, 1), (0, 1), (1, 2), (2, 0), (2, 1), (2, 2),
    (3, 0), (3, 1), (3, 2), (1, 3), (2, 3), (3, 3), (0, 2), (0, 3),
)


def staircase(step, column):
    rises = [(at, ORDER[at][column] - ORDER[at - 1][column]) for at in range(1, UNITS)]
    return sum(rise * ((step + 16 - at) // 16) for at, rise in rises if rise)


def unit_of(step):
    return staircase(step, 0), staircase(step, 1)


def places_on(kind, part):
    three = kind // 3
    two = kind // 2 - three
    one = kind - 2 * (kind // 2) - three
    return one * (3 - 2 * part) + two * (1 + 2 * part) + 2 * three


def kernel(
    idx_hbm, live_hbm, tok_hbm, wt_hbm, down_hbm, up_hbm, out_hbm,
    toks, wts, down, up, parts, relay, arrived, sums, final, upfin, out,
    idx_ref, live_ref, idx_all, idx_s, spread, transit, picked, zpicks, chosen, shr, shr_in,
    local_sem, out_sem, tok_s, tok_r, tokp_s, tokp_r, w_s, w_r,
    r1_s, r1_r, r2_s, r2_r, fin_s, fin_r,
    ixa_s, ixa_r, ixb_s, ixb_r, u1_s, u1_r, u2_s, u2_r, u3_s, u3_r, sh_s, sh_r,
):
    gx = lax.axis_index("gx")
    y = lax.axis_index("gy")
    gz = lax.axis_index("gz")
    z, x = gx // 4, gx % 4
    zh, core = gz // 2, gz % 2
    ring = zh * 4 + z

    def along_x(step):
        return (z * 4 + (x + step) % 4, y, gz)

    def along_y(step):
        return (gx, (y + step) % 4, gz)

    def along_z(step):
        return (((z + step) % 4) * 4 + x, y, gz)

    def on_ring(step):
        place = (ring + step) % 8
        return ((place % 4) * 4 + x, y, (place // 4) * 2 + core)

    partner = (gx, y, zh * 2 + 1 - core)

    def remote(src, dst, send, recv, to):
        return pltpu.make_async_remote_copy(
            src_ref=src, dst_ref=dst, send_sem=send, recv_sem=recv,
            device_id=to, device_id_type=pl.DeviceIdType.MESH,
        )

    def kind_of(way, part):
        return 1 if (way > 0) == (part == 0) else 2

    def tok_own(way, part):
        kind, block = kind_of(way, part), 2 * core + part
        return remote(
            toks.at[0, block], toks.at[kind, block],
            tok_s.at[kind - 1, part], tok_r.at[kind - 1, part], on_ring(way),
        )

    def tok_forward(part):
        block = 2 * core + part
        return remote(
            toks.at[1, block], toks.at[3, block],
            tok_s.at[2, part], tok_r.at[2, part], on_ring(1 if part == 0 else -1),
        )

    def tok_partner(kind, part, sent=True):
        block = 2 * (core if sent else 1 - core) + part
        return remote(
            toks.at[kind, block], toks.at[kind, block],
            tokp_s.at[kind - 1, part], tokp_r.at[kind - 1, part], partner,
        )

    def tok_arrival(kind, part):
        block = 2 * core + part
        return remote(
            toks.at[kind, block], toks.at[kind, block],
            tok_s.at[kind - 1, part], tok_r.at[kind - 1, part], partner,
        )

    def tok_partner_arrival(kind, part):
        return tok_partner(kind, part, False)

    def w_own(way, part):
        kind = kind_of(way, part)
        return remote(
            wts.at[0, part], wts.at[kind, part],
            w_s.at[kind - 1, part], w_r.at[kind - 1, part], along_x(way % 4),
        )

    def w_forward(part):
        return remote(
            wts.at[1, part], wts.at[3, part],
            w_s.at[2, part], w_r.at[2, part], along_x(1 if part == 0 else 3),
        )

    def w_arrival(kind, part):
        return remote(
            wts.at[kind, part], wts.at[kind, part],
            w_s.at[kind - 1, part], w_r.at[kind - 1, part], along_x(1),
        )

    def relay_copy(step, part):
        return remote(
            parts.at[step, (y + 2) % 4, part], relay.at[step, part],
            r1_s.at[step, part], r1_r.at[step, part], along_y(1 if part == 0 else 3),
        )

    def sum_copy(step, part):
        way = 1 if part == 0 else 3
        return remote(
            parts.at[step, (y + way) % 4], arrived.at[step, part],
            r2_s.at[step, part], r2_r.at[step, part], along_y(way),
        )

    def final_copy(step, part):
        rows, columns = unit_of(step)
        chunk = (x + places_on(columns, part)) % 4
        return remote(
            sums.at[step, part], final.at[z, chunk, part],
            fin_s.at[step, part], fin_r.at[z, chunk, part], along_z(places_on(rows, y % 2)),
        )

    def final_arrival(place, chunk, part):
        return remote(
            final.at[place, chunk, part], final.at[place, chunk, part],
            fin_s.at[0, part], fin_r.at[place, chunk, part], along_z(1),
        )

    def index_x(step):
        return remote(
            idx_all.at[z, x], idx_all.at[z, x], ixa_s.at[step - 1], ixa_r.at[step - 1], along_x(step)
        )

    def index_x_arrival(step):
        place = (x + 4 - step) % 4
        return remote(
            idx_all.at[z, place], idx_all.at[z, place],
            ixa_s.at[step - 1], ixa_r.at[step - 1], along_x(step),
        )

    def index_z(step):
        return remote(
            idx_all.at[z], idx_all.at[z], ixb_s.at[step - 1], ixb_r.at[step - 1], along_z(step)
        )

    def index_z_arrival(step):
        place = (z + 4 - step) % 4
        return remote(
            idx_all.at[place], idx_all.at[place],
            ixb_s.at[step - 1], ixb_r.at[step - 1], along_z(step),
        )

    def up_columns(step):
        return pl.ds(pl.multiple_of((x + step) % 4 * SLICE, SLICE), SLICE)

    def up_near(step):
        which = step // 2
        return remote(
            up.at[:, :, up_columns(step)], spread.at[x], u1_s.at[which], u1_r.at[which], along_x(step)
        )

    def up_near_arrival(step):
        which, place = step // 2, (x + 4 - step) % 4
        return remote(
            spread.at[place], spread.at[place], u1_s.at[which], u1_r.at[which], along_x(step)
        )

    def up_cross(part):
        return remote(
            up.at[pl.ds(2 * part, 2), :, up_columns(2)], transit.at[part],
            u1_s.at[2 + part], u1_r.at[2 + part], along_x(1 if part == 0 else 3),
        )

    def up_relay(part):
        step = 1 if part == 0 else 3
        place = (x + 4 - step) % 4
        return remote(
            transit.at[part], spread.at[place, pl.ds(2 * part, 2)],
            u1_s.at[4 + part], u1_r.at[4 + part], along_x(step),
        )

    mate = 1 - 2 * (z % 2)
    far = 3 - 2 * z

    def up_pair(part):
        chunk = z + mate if part == 0 else 3 - (z + mate)
        return remote(
            picked.at[chunk], zpicks.at[part], u2_s.at[part], u2_r.at[part], along_z(mate + 4)
        )

    def up_far():
        return remote(picked.at[3 - z], zpicks.at[2], u2_s.at[2], u2_r.at[2], along_z(far + 4))

    def up_last(step):
        return remote(
            chosen.at[(x + step) % 4], upfin.at[x], u3_s.at[step - 1], u3_r.at[step - 1], along_x(step)
        )

    def up_last_arrival(step):
        place = (x + 4 - step) % 4
        return remote(
            upfin.at[place], upfin.at[place], u3_s.at[step - 1], u3_r.at[step - 1], along_x(step)
        )

    def shrink_copy(step):
        return remote(
            shr.at[(y + step) % 4], shr_in.at[step - 1],
            sh_s.at[step - 1], sh_r.at[step - 1], along_y(step),
        )

    loads = [
        pltpu.make_async_copy(idx_hbm, idx_ref, local_sem.at[4]),
        pltpu.make_async_copy(tok_hbm, toks.at[0], local_sem.at[0]),
        pltpu.make_async_copy(wt_hbm, wts.at[0], local_sem.at[1]),
        pltpu.make_async_copy(down_hbm, down, local_sem.at[2]),
        pltpu.make_async_copy(up_hbm, up, local_sem.at[3]),
        pltpu.make_async_copy(live_hbm, live_ref, local_sem.at[5]),
    ]
    for load in loads:
        load.start()
    barrier = pltpu.get_barrier_semaphore()
    peers = [along_x(n) for n in (1, 2, 3)] + [along_y(n) for n in (1, 2, 3)]
    peers += [along_z(n) for n in (1, 2, 3)] + [on_ring(1), on_ring(-1), partner]
    for peer in peers:
        pl.semaphore_signal(barrier, inc=1, device_id=peer, device_id_type=pl.DeviceIdType.MESH)

    loads[0].wait()
    lane = lax.broadcasted_iota(jnp.int32, (1, 128), 1)
    row = jnp.zeros((1, 128), jnp.int32)
    for block in range(4):
        row = jnp.where(lane == block, idx_ref[block], row)
    idx_all[z, x] = row
    loads[1].wait()
    loads[2].wait()
    pl.semaphore_wait(barrier, len(peers))

    for n in (1, 2, 3):
        index_x(n).start()
    for way, order in ((1, (0, 1)), (-1, (1, 0))):
        for part in order:
            w_own(way, part).start()
            tok_own(way, part).start()

    def step_body(step, carry):
        @pl.when(step == 1)
        def _():
            loads[3].wait()
            for block in range(4):
                chosen_down = down[idx_ref[block]]
                shr[block] = lax.dot_general(
                    chosen_down, toks[0, block], LAST, preferred_element_type=F32
                )
            for n in (1, 2, 3):
                index_x_arrival(n).wait_recv()
            for n in (1, 2, 3):
                index_z(n).start()
                shrink_copy(n).start()
            for part in (0, 1):
                tok_arrival(1, part).wait_recv()
                tok_partner(1, part).start()
            for part in (0, 1):
                tok_partner_arrival(1, part).wait_recv()

        @pl.when(step == 2)
        def _():
            for part in (0, 1):
                w_arrival(1, part).wait_recv()

        @pl.when(step == 4)
        def _():
            for part in (0, 1):
                tok_arrival(2, part).wait_recv()
                tok_forward(part).start()
                tok_partner(2, part).start()
            loads[4].wait()
            for part in (0, 1):
                w_arrival(2, part).wait_recv()
            for part in (0, 1):
                up_near(1 + 2 * part).start()
                up_cross(part).start()

        @pl.when(step == 5)
        def _():
            for part in (0, 1):
                tok_partner_arrival(2, part).wait_recv()

        @pl.when(step == 6)
        def _():
            for part in (0, 1):
                up_cross(part).wait_recv()
                up_relay(part).start()
            for part in (0, 1):
                w_forward(part).start()

        @pl.when(step == 7)
        def _():
            for part in (0, 1):
                tok_arrival(3, part).wait_recv()
                tok_partner(3, part).start()

        @pl.when(step == 8)
        def _():
            for part in (0, 1):
                tok_partner_arrival(3, part).wait_recv()

        @pl.when(step == 11)
        def _():
            for part in (0, 1):
                w_arrival(3, part).wait_recv()

        @pl.when(step < UNITS)
        def _():
            s, t = unit_of(step)
            result = lax.dot_general(
                wts[t].reshape(COLS, WIDTH), toks[s].reshape(4 * BLOCK, WIDTH), LAST,
                preferred_element_type=F32,
            ).astype(BF)
            for block in range(4):
                tile = result[:, block * BLOCK : (block + 1) * BLOCK]
                parts[step, block] = tile.reshape(2, HALF, BLOCK)

        @pl.when((step >= LAG_RELAY) & (step < UNITS + LAG_RELAY))
        def _():
            done = step - LAG_RELAY
            for part in (0, 1):
                to = (y + (1 if part == 0 else 3)) % 4
                relay_copy(done, part).wait_recv()
                added = parts[done, to, part].astype(F32) + relay[done, part].astype(F32)
                parts[done, to, part] = added.astype(BF)

        @pl.when(step < UNITS)
        def _():
            for part in (0, 1):
                relay_copy(step, part).start()

        @pl.when((step >= LAG_RELAY) & (step < UNITS + LAG_RELAY))
        def _():
            for part in (0, 1):
                sum_copy(step - LAG_RELAY, part).start()

        @pl.when(step >= LAG_SUM)
        def _():
            done = step - LAG_SUM
            rows, columns = unit_of(done)
            for part in (0, 1):
                sum_copy(done, part).wait_recv()
            total = parts[done, y].astype(F32) + arrived[done, 0].astype(F32)
            total = (total + arrived[done, 1].astype(F32)).astype(BF)

            @pl.when(rows == 0)
            def _():
                for part in (0, 1):
                    final[z, (x + places_on(columns, part)) % 4, part] = total[part]

            @pl.when(rows > 0)
            def _():
                sums[done] = total
                for part in (0, 1):
                    final_copy(done, part).start()

        @pl.when(step == PICK_STEP)
        def _():
            for n in (1, 2, 3):
                index_z_arrival(n).wait_recv()
            to_scalars = pltpu.make_async_copy(idx_all, idx_s, local_sem.at[0])
            to_scalars.start()
            own = pltpu.make_async_copy(
                up.at[:, :, pl.ds(pl.multiple_of(x * SLICE, SLICE), SLICE)], spread.at[x], local_sem.at[1]
            )
            own.start()
            for part in (0, 1):
                up_near_arrival(1 + 2 * part).wait_recv()
                up_relay(part).wait_recv()
            to_scalars.wait()
            own.wait()
            for to_z in range(4):
                for to_x in range(4):
                    local = idx_s[to_z, to_x, 0, y] - 16 * z
                    owned = jnp.where((local >= 0) & (local < 16), 1.0, 0.0).astype(F32)
                    kept = jnp.clip(local, 0, 15)
                    factor = spread[kept // 4, kept % 4].astype(F32) * owned
                    picked[to_z, to_x] = factor.astype(BF)
            for part in (1, 0):
                up_pair(part).start()

        @pl.when(step == PAIR_STEP)
        def _():
            up_pair(1).wait_recv()
            for to_x in range(4):
                picked[3 - z, to_x] = picked[3 - z, to_x] + zpicks[1, to_x]
            up_far().start()

        @pl.when(step == FAR_STEP)
        def _():
            up_pair(0).wait_recv()
            up_far().wait_recv()
            for to_x in range(4):
                chosen[to_x] = (picked[z, to_x] + zpicks[0, to_x]) + zpicks[2, to_x]
            for n in (1, 2, 3):
                up_last(n).start()
            upfin[x] = chosen[x]

        return carry

    lax.fori_loop(0, UNITS + LAG_SUM, step_body, 0)

    def finish_sends():
        for n in (1, 2, 3):
            index_x(n).wait_send()
            index_z(n).wait_send()
            up_last(n).wait_send()
            shrink_copy(n).wait_send()
        up_pair(0).wait_send()
        up_pair(1).wait_send()
        up_far().wait_send()
        for part in (0, 1):
            for way in (1, -1):
                w_own(way, part).wait_send()
                tok_own(way, part).wait_send()
            w_forward(part).wait_send()
            tok_forward(part).wait_send()
            up_near(1 + 2 * part).wait_send()
            up_cross(part).wait_send()
            up_relay(part).wait_send()
            for kind in (1, 2, 3):
                tok_partner(kind, part).wait_send()

        def drain(step, carry):
            for part in (0, 1):
                relay_copy(step, part).wait_send()
                sum_copy(step, part).wait_send()

                @pl.when(unit_of(step)[0] > 0)
                def _():
                    final_copy(step, part).wait_send()

            return carry

        lax.fori_loop(0, UNITS, drain, 0)

    for n in (1, 2, 3):
        shrink_copy(n).wait_recv()
    low = (shr[y] + shr_in[0] + (shr_in[1] + shr_in[2])).astype(BF)
    same = lax.broadcasted_iota(jnp.int32, (BLOCK, BLOCK), 0) == lax.broadcasted_iota(
        jnp.int32, (BLOCK, BLOCK), 1
    )
    eye = jnp.where(same, 1.0, 0.0).astype(BF)
    turned = lax.dot_general(eye, low, LAST, preferred_element_type=F32)
    doubled = (2.0 * turned).astype(BF)
    loads[5].wait()
    live = lax.broadcasted_iota(jnp.int32, (BLOCK, 1), 0) < live_ref[y]
    for n in (1, 2, 3):
        up_last_arrival(n).wait_recv()

    def write_out(n):
        place = (z + n) % 4
        columns = pl.ds(pl.multiple_of(place * SLICE, SLICE), SLICE)
        return pltpu.make_async_copy(out.at[n], out_hbm.at[:, columns], out_sem.at[n])

    for n in (0, 1, 3, 2):
        place = (z + n) % 4
        if n:
            for chunk in range(4):
                for part in (0, 1):
                    final_arrival(place, chunk, part).wait_recv()
        base = lax.dot_general(
            eye, final[place].reshape(SLICE, BLOCK), LAST, preferred_element_type=F32
        )
        extra = jnp.dot(doubled, upfin[place], preferred_element_type=F32)
        out[n] = jnp.where(live, base + extra, 0.0).astype(BF)
        write_out(n).start()
        if n == 0:
            finish_sends()
    for n in range(4):
        write_out(n).wait()


def body(tokens, base_up_weight, adapter_down_weight, adapter_up_weight, block_adapter_index, request_rows):
    dma = pltpu.SemaphoreType.DMA
    half_tile = (2, HALF, BLOCK)
    any_space = pl.BlockSpec(memory_space=pl.ANY)
    return pl.pallas_call(
        kernel,
        out_shape=jax.ShapeDtypeStruct((BLOCK, 4 * SLICE), BF),
        in_specs=[any_space] * 6,
        out_specs=any_space,
        scratch_shapes=[
            pltpu.VMEM((4, 4, BLOCK, WIDTH), BF),
            pltpu.VMEM((4, 2, HALF, WIDTH), BF),
            pltpu.VMEM((CATALOG, RANK, WIDTH), BF),
            pltpu.VMEM((4, RANK, 4 * SLICE), BF),
            pltpu.VMEM((UNITS, 4, *half_tile), BF),
            pltpu.VMEM((UNITS, *half_tile), BF),
            pltpu.VMEM((UNITS, 2, *half_tile), BF),
            pltpu.VMEM((UNITS, *half_tile), BF),
            pltpu.VMEM((4, 4, *half_tile), BF),
            pltpu.VMEM((4, RANK, SLICE), BF),
            pltpu.VMEM((4, BLOCK, SLICE), BF),
            pltpu.SMEM((4,), jnp.int32),
            pltpu.SMEM((4,), jnp.int32),
            pltpu.VMEM((4, 4, 1, 128), jnp.int32),
            pltpu.SMEM((4, 4, 1, 128), jnp.int32),
            pltpu.VMEM((4, 4, RANK, SLICE), BF),
            pltpu.VMEM((2, 2, RANK, SLICE), BF),
            pltpu.VMEM((4, 4, RANK, SLICE), BF),
            pltpu.VMEM((3, 4, RANK, SLICE), BF),
            pltpu.VMEM((4, RANK, SLICE), BF),
            pltpu.VMEM((4, RANK, BLOCK), F32),
            pltpu.VMEM((3, RANK, BLOCK), F32),
            dma((6,)), dma((4,)),
            dma((3, 2)), dma((3, 2)), dma((3, 2)), dma((3, 2)), dma((3, 2)), dma((3, 2)),
            dma((UNITS, 2)), dma((UNITS, 2)), dma((UNITS, 2)), dma((UNITS, 2)),
            dma((UNITS, 2)), dma((4, 4, 2)),
            dma((3,)), dma((3,)), dma((3,)), dma((3,)),
            dma((6,)), dma((6,)), dma((3,)), dma((3,)), dma((3,)), dma((3,)),
            dma((3,)), dma((3,)),
        ],
        compiler_params=pltpu.CompilerParams(
            collective_id=0, has_side_effects=True, vmem_limit_bytes=67043328
        ),
    )(
        block_adapter_index,
        request_rows,
        tokens.reshape(4, BLOCK, WIDTH),
        base_up_weight.T.reshape(2, HALF, WIDTH),
        adapter_down_weight,
        adapter_up_weight,
    )


def solution(mesh):
    in_specs = (
        P("gx", "gy"),
        P("gy", ("gz", "gx")),
        P(None, None, "gy"),
        P("gx", None, "gz"),
        P("gx"),
        P("gx"),
    )
    out_specs = P(("gx", "gy"), "gz")
    return jax.shard_map(body, mesh=mesh, in_specs=in_specs, out_specs=out_specs, check_vma=False)
```

```python
import functools

import jax
import jax.numpy as jnp
from jax import lax
from jax.experimental import pallas as pl
from jax.experimental.pallas import tpu as pltpu
from jax.sharding import PartitionSpec as P

BLOCK = 128
RANK = 16
CATALOG = 64
WIDTH = 1152
COLS = 288
HALF = COLS // 2
SLICE = 4 * COLS
UNITS = 16
LAG_RELAY = 2
LAG_SUM = 4
PICK_STEP = 6
PAIR_STEP = 8
FAR_STEP = 12
BF = jnp.bfloat16
F32 = jnp.float32
LAST = (((1,), (1,)), ((), ()))


ORDER = (
    (0, 0), (0, 1), (1, 0), (1, 1), (2, 0), (2, 1), (1, 2), (3, 0),
    (2, 2), (3, 1), (1, 3), (3, 2), (2, 3), (3, 3), (0, 2), (0, 3),
)


def staircase(step, column):
    rises = [(at, ORDER[at][column] - ORDER[at - 1][column]) for at in range(1, UNITS)]
    return sum(rise * ((step + 16 - at) // 16) for at, rise in rises if rise)


def unit_of(step):
    return staircase(step, 0), staircase(step, 1)


def places_on(kind, part):
    three = kind // 3
    two = kind // 2 - three
    one = kind - 2 * (kind // 2) - three
    return one * (3 - 2 * part) + two * (1 + 2 * part) + 2 * three


def kernel(
    idx_hbm, live_hbm, tok_hbm, wt_hbm, down_hbm, up_hbm, out_hbm,
    toks, wts, down, up, parts, relay, arrived, sums, final, upfin, out,
    idx_ref, live_ref, idx_all, idx_s, spread, transit, picked, zpicks, chosen, shr, shr_in,
    local_sem, out_sem, tok_s, tok_r, tokp_s, tokp_r, w_s, w_r,
    r1_s, r1_r, r2_s, r2_r, fin_s, fin_r,
    ixa_s, ixa_r, ixb_s, ixb_r, u1_s, u1_r, u2_s, u2_r, u3_s, u3_r, sh_s, sh_r,
):
    gx = lax.axis_index("gx")
    y = lax.axis_index("gy")
    gz = lax.axis_index("gz")
    z, x = gx // 4, gx % 4
    zh, core = gz // 2, gz % 2
    ring = zh * 4 + z

    def along_x(step):
        return (z * 4 + (x + step) % 4, y, gz)

    def along_y(step):
        return (gx, (y + step) % 4, gz)

    def along_z(step):
        return (((z + step) % 4) * 4 + x, y, gz)

    def on_ring(step):
        place = (ring + step) % 8
        return ((place % 4) * 4 + x, y, (place // 4) * 2 + core)

    partner = (gx, y, zh * 2 + 1 - core)

    def remote(src, dst, send, recv, to):
        return pltpu.make_async_remote_copy(
            src_ref=src, dst_ref=dst, send_sem=send, recv_sem=recv,
            device_id=to, device_id_type=pl.DeviceIdType.MESH,
        )

    def kind_of(way, part):
        return 1 if (way > 0) == (part == 0) else 2

    def tok_own(way, part):
        kind, block = kind_of(way, part), 2 * core + part
        return remote(
            toks.at[0, block], toks.at[kind, block],
            tok_s.at[kind - 1, part], tok_r.at[kind - 1, part], on_ring(way),
        )

    def tok_forward(part):
        block = 2 * core + part
        return remote(
            toks.at[1, block], toks.at[3, block],
            tok_s.at[2, part], tok_r.at[2, part], on_ring(1 if part == 0 else -1),
        )

    def tok_partner(kind, part, sent=True):
        block = 2 * (core if sent else 1 - core) + part
        return remote(
            toks.at[kind, block], toks.at[kind, block],
            tokp_s.at[kind - 1, part], tokp_r.at[kind - 1, part], partner,
        )

    def tok_arrival(kind, part):
        block = 2 * core + part
        return remote(
            toks.at[kind, block], toks.at[kind, block],
            tok_s.at[kind - 1, part], tok_r.at[kind - 1, part], partner,
        )

    def tok_partner_arrival(kind, part):
        return tok_partner(kind, part, False)

    def w_own(way, part):
        kind = kind_of(way, part)
        return remote(
            wts.at[0, part], wts.at[kind, part],
            w_s.at[kind - 1, part], w_r.at[kind - 1, part], along_x(way % 4),
        )

    def w_forward(part):
        return remote(
            wts.at[1, part], wts.at[3, part],
            w_s.at[2, part], w_r.at[2, part], along_x(1 if part == 0 else 3),
        )

    def w_arrival(kind, part):
        return remote(
            wts.at[kind, part], wts.at[kind, part],
            w_s.at[kind - 1, part], w_r.at[kind - 1, part], along_x(1),
        )

    def relay_copy(step, part):
        return remote(
            parts.at[step, (y + 2) % 4, part], relay.at[step, part],
            r1_s.at[step, part], r1_r.at[step, part], along_y(1 if part == 0 else 3),
        )

    def sum_copy(step, part):
        way = 1 if part == 0 else 3
        return remote(
            parts.at[step, (y + way) % 4], arrived.at[step, part],
            r2_s.at[step, part], r2_r.at[step, part], along_y(way),
        )

    def final_copy(step, part):
        rows, columns = unit_of(step)
        chunk = (x + places_on(columns, part)) % 4
        return remote(
            sums.at[step, part], final.at[z, chunk, part],
            fin_s.at[step, part], fin_r.at[z, chunk, part], along_z(places_on(rows, y % 2)),
        )

    def final_arrival(place, chunk, part):
        return remote(
            final.at[place, chunk, part], final.at[place, chunk, part],
            fin_s.at[0, part], fin_r.at[place, chunk, part], along_z(1),
        )

    def index_x(step):
        return remote(
            idx_all.at[z, x], idx_all.at[z, x], ixa_s.at[step - 1], ixa_r.at[step - 1], along_x(step)
        )

    def index_x_arrival(step):
        place = (x + 4 - step) % 4
        return remote(
            idx_all.at[z, place], idx_all.at[z, place],
            ixa_s.at[step - 1], ixa_r.at[step - 1], along_x(step),
        )

    def index_z(step):
        return remote(
            idx_all.at[z], idx_all.at[z], ixb_s.at[step - 1], ixb_r.at[step - 1], along_z(step)
        )

    def index_z_arrival(step):
        place = (z + 4 - step) % 4
        return remote(
            idx_all.at[place], idx_all.at[place],
            ixb_s.at[step - 1], ixb_r.at[step - 1], along_z(step),
        )

    def up_columns(step):
        return pl.ds(pl.multiple_of((x + step) % 4 * SLICE, SLICE), SLICE)

    def up_near(step):
        which = step // 2
        return remote(
            up.at[:, :, up_columns(step)], spread.at[x], u1_s.at[which], u1_r.at[which], along_x(step)
        )

    def up_near_arrival(step):
        which, place = step // 2, (x + 4 - step) % 4
        return remote(
            spread.at[place], spread.at[place], u1_s.at[which], u1_r.at[which], along_x(step)
        )

    def up_cross(part):
        return remote(
            up.at[pl.ds(2 * part, 2), :, up_columns(2)], transit.at[part],
            u1_s.at[2 + part], u1_r.at[2 + part], along_x(1 if part == 0 else 3),
        )

    def up_relay(part):
        step = 1 if part == 0 else 3
        place = (x + 4 - step) % 4
        return remote(
            transit.at[part], spread.at[place, pl.ds(2 * part, 2)],
            u1_s.at[4 + part], u1_r.at[4 + part], along_x(step),
        )

    mate = 1 - 2 * (z % 2)
    far = 3 - 2 * z

    def up_pair(part):
        chunk = z + mate if part == 0 else 3 - (z + mate)
        return remote(
            picked.at[chunk], zpicks.at[part], u2_s.at[part], u2_r.at[part], along_z(mate + 4)
        )

    def up_far():
        return remote(picked.at[3 - z], zpicks.at[2], u2_s.at[2], u2_r.at[2], along_z(far + 4))

    def up_last(step):
        return remote(
            chosen.at[(x + step) % 4], upfin.at[x], u3_s.at[step - 1], u3_r.at[step - 1], along_x(step)
        )

    def up_last_arrival(step):
        place = (x + 4 - step) % 4
        return remote(
            upfin.at[place], upfin.at[place], u3_s.at[step - 1], u3_r.at[step - 1], along_x(step)
        )

    def shrink_copy(step):
        return remote(
            shr.at[(y + step) % 4], shr_in.at[step - 1],
            sh_s.at[step - 1], sh_r.at[step - 1], along_y(step),
        )

    loads = [
        pltpu.make_async_copy(idx_hbm, idx_ref, local_sem.at[4]),
        pltpu.make_async_copy(tok_hbm, toks.at[0], local_sem.at[0]),
        pltpu.make_async_copy(wt_hbm, wts.at[0], local_sem.at[1]),
        pltpu.make_async_copy(down_hbm, down, local_sem.at[2]),
        pltpu.make_async_copy(up_hbm, up, local_sem.at[3]),
        pltpu.make_async_copy(live_hbm, live_ref, local_sem.at[5]),
    ]
    for load in loads:
        load.start()
    barrier = pltpu.get_barrier_semaphore()
    peers = [along_x(n) for n in (1, 2, 3)] + [along_y(n) for n in (1, 2, 3)]
    peers += [along_z(n) for n in (1, 2, 3)] + [on_ring(1), on_ring(-1), partner]
    for peer in peers:
        pl.semaphore_signal(barrier, inc=1, device_id=peer, device_id_type=pl.DeviceIdType.MESH)

    loads[0].wait()
    lane = lax.broadcasted_iota(jnp.int32, (1, 128), 1)
    row = jnp.zeros((1, 128), jnp.int32)
    for block in range(4):
        row = jnp.where(lane == block, idx_ref[block], row)
    idx_all[z, x] = row
    loads[1].wait()
    loads[2].wait()
    pl.semaphore_wait(barrier, len(peers))

    for n in (1, 2, 3):
        index_x(n).start()
    for way in (1, -1):
        w_own(way, 0 if way > 0 else 1).start()
        tok_own(way, 0 if way > 0 else 1).start()
    for way in (1, -1):
        tok_own(way, 1 if way > 0 else 0).start()

    def step_body(step, carry):
        @pl.when((step >= LAG_RELAY) & (step < UNITS + LAG_RELAY))
        def _():
            done = step - LAG_RELAY
            for part in (0, 1):
                to = (y + (1 if part == 0 else 3)) % 4
                relay_copy(done, part).wait_recv()
                added = parts[done, to, part].astype(F32) + relay[done, part].astype(F32)
                parts[done, to, part] = added.astype(BF)

        @pl.when((step >= LAG_RELAY) & (step < UNITS + LAG_RELAY))
        def _():
            for part in (0, 1):
                sum_copy(step - LAG_RELAY, part).start()

        @pl.when(step >= LAG_SUM)
        def _():
            done = step - LAG_SUM
            rows, columns = unit_of(done)
            for part in (0, 1):
                sum_copy(done, part).wait_recv()
            total = parts[done, y].astype(F32) + arrived[done, 0].astype(F32)
            total = (total + arrived[done, 1].astype(F32)).astype(BF)

            @pl.when(rows == 0)
            def _():
                for part in (0, 1):
                    final[z, (x + places_on(columns, part)) % 4, part] = total[part]

            @pl.when(rows > 0)
            def _():
                sums[done] = total
                for part in (0, 1):
                    final_copy(done, part).start()

        @pl.when(step == 1)
        def _():
            loads[3].wait()
            for block in range(4):
                chosen_down = down[idx_ref[block]]
                shr[block] = lax.dot_general(
                    chosen_down, toks[0, block], LAST, preferred_element_type=F32
                )
            for n in (1, 2, 3):
                shrink_copy(n).start()
            for n in (1, 2, 3):
                index_x_arrival(n).wait_recv()
            for n in (1, 2, 3):
                index_z(n).start()

        @pl.when(step == 1)
        def _():
            loads[4].wait()
            for way in (1, -1):
                part = 0 if way > 0 else 1
                w_own(way, part).wait_send()
                up_near(way % 4).start()
                up_cross(part).start()
            for part in (0, 1):
                tok_arrival(1, part).wait_recv()
                tok_partner(1, part).start()
            for part in (0, 1):
                w_arrival(1, part).wait_recv()

        @pl.when(step == 2)
        def _():
            for way in (1, -1):
                part = 0 if way > 0 else 1
                up_near(way % 4).wait_send()
                up_cross(part).wait_send()
                w_own(way, 1 - part).start()
            for part in (0, 1):
                tok_partner_arrival(1, part).wait_recv()

        @pl.when(step == 3)
        def _():
            for way in (1, -1):
                part = 0 if way > 0 else 1
                tok_own(way, 1 - part).wait_send()
                tok_forward(part).start()

        @pl.when(step == 4)
        def _():
            for part in (0, 1):
                tok_partner_arrival(2, part).wait_recv()

        @pl.when(step == 6)
        def _():
            for part in (0, 1):
                w_arrival(2, part).wait_recv()
                w_forward(part).start()
            for part in (0, 1):
                tok_arrival(3, part).wait_recv()
                tok_partner(3, part).start()

        @pl.when(step == 7)
        def _():
            for part in (0, 1):
                tok_partner_arrival(3, part).wait_recv()

        @pl.when(step == 10)
        def _():
            for part in (0, 1):
                w_arrival(3, part).wait_recv()

        @pl.when(step < UNITS)
        def _():
            s, t = unit_of(step)
            result = lax.dot_general(
                wts[t].reshape(COLS, WIDTH), toks[s].reshape(4 * BLOCK, WIDTH), LAST,
                preferred_element_type=F32,
            ).astype(BF)
            for block in range(4):
                tile = result[:, block * BLOCK : (block + 1) * BLOCK]
                parts[step, block] = tile.reshape(2, HALF, BLOCK)

        @pl.when(step < UNITS)
        def _():
            for part in (0, 1):
                relay_copy(step, part).start()

        @pl.when(step == 3)
        def _():
            for part in (0, 1):
                tok_arrival(2, part).wait_recv()
                tok_partner(2, part).start()
            for part in (0, 1):
                up_cross(part).wait_recv()
                up_relay(part).start()

        @pl.when(step == PICK_STEP)
        def _():
            for n in (1, 2, 3):
                index_z_arrival(n).wait_recv()
            to_scalars = pltpu.make_async_copy(idx_all, idx_s, local_sem.at[0])
            to_scalars.start()
            own = pltpu.make_async_copy(
                up.at[:, :, pl.ds(pl.multiple_of(x * SLICE, SLICE), SLICE)], spread.at[x], local_sem.at[1]
            )
            own.start()
            for part in (0, 1):
                up_near_arrival(1 + 2 * part).wait_recv()
                up_relay(part).wait_recv()
            to_scalars.wait()
            own.wait()
            for to_z in range(4):
                for to_x in range(4):
                    local = idx_s[to_z, to_x, 0, y] - 16 * z
                    owned = jnp.where((local >= 0) & (local < 16), 1.0, 0.0).astype(F32)
                    kept = jnp.clip(local, 0, 15)
                    factor = spread[kept // 4, kept % 4].astype(F32) * owned
                    picked[to_z, to_x] = factor.astype(BF)
            for part in (1, 0):
                up_pair(part).start()

        @pl.when(step == PAIR_STEP)
        def _():
            up_pair(1).wait_recv()
            for to_x in range(4):
                picked[3 - z, to_x] = picked[3 - z, to_x] + zpicks[1, to_x]
            up_far().start()

        @pl.when(step == FAR_STEP)
        def _():
            up_pair(0).wait_recv()
            up_far().wait_recv()
            for to_x in range(4):
                chosen[to_x] = (picked[z, to_x] + zpicks[0, to_x]) + zpicks[2, to_x]
            for n in (1, 2, 3):
                up_last(n).start()
            upfin[x] = chosen[x]

        return carry

    lax.fori_loop(0, UNITS + LAG_SUM, step_body, 0)

    def finish_sends():
        for n in (1, 2, 3):
            index_x(n).wait_send()
            index_z(n).wait_send()
            up_last(n).wait_send()
            shrink_copy(n).wait_send()
        up_pair(0).wait_send()
        up_pair(1).wait_send()
        up_far().wait_send()
        for part in (0, 1):
            way = 1 if part == 0 else -1
            w_own(way, 1 - part).wait_send()
            tok_own(way, part).wait_send()
            w_forward(part).wait_send()
            tok_forward(part).wait_send()
            up_relay(part).wait_send()
            for kind in (1, 2, 3):
                tok_partner(kind, part).wait_send()

        def drain(step, carry):
            for part in (0, 1):
                relay_copy(step, part).wait_send()
                sum_copy(step, part).wait_send()

                @pl.when(unit_of(step)[0] > 0)
                def _():
                    final_copy(step, part).wait_send()

            return carry

        lax.fori_loop(0, UNITS, drain, 0)

    for n in (1, 2, 3):
        shrink_copy(n).wait_recv()
    low = (shr[y] + shr_in[0] + (shr_in[1] + shr_in[2])).astype(BF)
    same = lax.broadcasted_iota(jnp.int32, (BLOCK, BLOCK), 0) == lax.broadcasted_iota(
        jnp.int32, (BLOCK, BLOCK), 1
    )
    eye = jnp.where(same, 1.0, 0.0).astype(BF)
    turned = lax.dot_general(eye, low, LAST, preferred_element_type=F32)
    doubled = (2.0 * turned).astype(BF)
    loads[5].wait()
    live = lax.broadcasted_iota(jnp.int32, (BLOCK, 1), 0) < live_ref[y]
    for n in (1, 2, 3):
        up_last_arrival(n).wait_recv()

    def write_out(n):
        place = (z + n) % 4
        columns = pl.ds(pl.multiple_of(place * SLICE, SLICE), SLICE)
        return pltpu.make_async_copy(out.at[n], out_hbm.at[:, columns], out_sem.at[n])

    for n in (0, 1, 3, 2):
        place = (z + n) % 4
        if n:
            for chunk in range(4):
                for part in (0, 1):
                    final_arrival(place, chunk, part).wait_recv()
        base = lax.dot_general(
            eye, final[place].reshape(SLICE, BLOCK), LAST, preferred_element_type=F32
        )
        extra = jnp.dot(doubled, upfin[place], preferred_element_type=F32)
        out[n] = jnp.where(live, base + extra, 0.0).astype(BF)
        write_out(n).start()
        if n == 0:
            finish_sends()
    for n in range(4):
        write_out(n).wait()


def body(tokens, base_up_weight, adapter_down_weight, adapter_up_weight, block_adapter_index, request_rows):
    dma = pltpu.SemaphoreType.DMA
    half_tile = (2, HALF, BLOCK)
    any_space = pl.BlockSpec(memory_space=pl.ANY)
    return pl.pallas_call(
        kernel,
        out_shape=jax.ShapeDtypeStruct((BLOCK, 4 * SLICE), BF),
        in_specs=[any_space] * 6,
        out_specs=any_space,
        scratch_shapes=[
            pltpu.VMEM((4, 4, BLOCK, WIDTH), BF),
            pltpu.VMEM((4, 2, HALF, WIDTH), BF),
            pltpu.VMEM((CATALOG, RANK, WIDTH), BF),
            pltpu.VMEM((4, RANK, 4 * SLICE), BF),
            pltpu.VMEM((UNITS, 4, *half_tile), BF),
            pltpu.VMEM((UNITS, *half_tile), BF),
            pltpu.VMEM((UNITS, 2, *half_tile), BF),
            pltpu.VMEM((UNITS, *half_tile), BF),
            pltpu.VMEM((4, 4, *half_tile), BF),
            pltpu.VMEM((4, RANK, SLICE), BF),
            pltpu.VMEM((4, BLOCK, SLICE), BF),
            pltpu.SMEM((4,), jnp.int32),
            pltpu.SMEM((4,), jnp.int32),
            pltpu.VMEM((4, 4, 1, 128), jnp.int32),
            pltpu.SMEM((4, 4, 1, 128), jnp.int32),
            pltpu.VMEM((4, 4, RANK, SLICE), BF),
            pltpu.VMEM((2, 2, RANK, SLICE), BF),
            pltpu.VMEM((4, 4, RANK, SLICE), BF),
            pltpu.VMEM((3, 4, RANK, SLICE), BF),
            pltpu.VMEM((4, RANK, SLICE), BF),
            pltpu.VMEM((4, RANK, BLOCK), F32),
            pltpu.VMEM((3, RANK, BLOCK), F32),
            dma((6,)), dma((4,)),
            dma((3, 2)), dma((3, 2)), dma((3, 2)), dma((3, 2)), dma((3, 2)), dma((3, 2)),
            dma((UNITS, 2)), dma((UNITS, 2)), dma((UNITS, 2)), dma((UNITS, 2)),
            dma((UNITS, 2)), dma((4, 4, 2)),
            dma((3,)), dma((3,)), dma((3,)), dma((3,)),
            dma((6,)), dma((6,)), dma((3,)), dma((3,)), dma((3,)), dma((3,)),
            dma((3,)), dma((3,)),
        ],
        compiler_params=pltpu.CompilerParams(
            collective_id=0, has_side_effects=True, vmem_limit_bytes=67043328
        ),
    )(
        block_adapter_index,
        request_rows,
        tokens.reshape(4, BLOCK, WIDTH),
        base_up_weight.T.reshape(2, HALF, WIDTH),
        adapter_down_weight,
        adapter_up_weight,
    )


def solution(mesh):
    in_specs = (
        P("gx", "gy"),
        P("gy", ("gz", "gx")),
        P(None, None, "gy"),
        P("gx", None, "gz"),
        P("gx"),
        P("gx"),
    )
    out_specs = P(("gx", "gy"), "gz")
    return jax.shard_map(body, mesh=mesh, in_specs=in_specs, out_specs=out_specs, check_vma=False)
```

```python
import functools

import jax
import jax.numpy as jnp
from jax import lax
from jax.experimental import pallas as pl
from jax.experimental.pallas import tpu as pltpu
from jax.sharding import PartitionSpec as P

BLOCK = 128
RANK = 16
CATALOG = 64
WIDTH = 1152
COLS = 288
HALF = COLS // 2
SLICE = 4 * COLS
UNITS = 16
LAG_RELAY = 2
LAG_SUM = 4
PICK_STEP = 6
PAIR_STEP = 9
FAR_STEP = 15
AWAY = (2, 12)
BF = jnp.bfloat16
F32 = jnp.float32
LAST = (((1,), (1,)), ((), ()))


ORDER = (
    (0, 0), (0, 1), (1, 0), (1, 1), (2, 0), (2, 1), (1, 2), (3, 0),
    (2, 2), (3, 1), (1, 3), (3, 2), (2, 3), (3, 3), (0, 2), (0, 3),
)


def staircase(step, column):
    rises = [(at, ORDER[at][column] - ORDER[at - 1][column]) for at in range(1, UNITS)]
    return sum(rise * ((step + 16 - at) // 16) for at, rise in rises if rise)


def unit_of(step):
    return staircase(step, 0), staircase(step, 1)


def places_on(kind, part):
    three = kind // 3
    two = kind // 2 - three
    one = kind - 2 * (kind // 2) - three
    return one * (3 - 2 * part) + two * (1 + 2 * part) + 2 * three


def kernel(
    idx_hbm, live_hbm, tok_hbm, wt_hbm, down_hbm, up_hbm, out_ref,
    toks, wts, down, up, parts, relay, arrived, sums, final, upfin,
    idx_ref, live_ref, idx_all, idx_s, spread, transit, picked, zpicks, chosen, shr, shr_in,
    local_sem, one, tok_s, tok_r, tokp_r, w_s, w_r, r1_r, r2_r, fin_r, u2_r,
):
    gx = lax.axis_index("gx")
    y = lax.axis_index("gy")
    gz = lax.axis_index("gz")
    z, x = gx // 4, gx % 4
    zh, core = gz // 2, gz % 2
    ring = zh * 4 + z

    def along_x(step):
        return (z * 4 + (x + step) % 4, y, gz)

    def along_y(step):
        return (gx, (y + step) % 4, gz)

    def along_z(step):
        return (((z + step) % 4) * 4 + x, y, gz)

    def on_ring(step):
        place = (ring + step) % 8
        return ((place % 4) * 4 + x, y, (place // 4) * 2 + core)

    partner = (gx, y, zh * 2 + 1 - core)

    def remote(src, dst, send, recv, to):
        return pltpu.make_async_remote_copy(
            src_ref=src, dst_ref=dst, send_sem=send, recv_sem=recv,
            device_id=to, device_id_type=pl.DeviceIdType.MESH,
        )

    def kind_of(way, part):
        return 1 if (way > 0) == (part == 0) else 2

    def tok_own(way, part):
        kind, block = kind_of(way, part), 2 * core + part
        return remote(
            toks.at[0, block], toks.at[kind, block],
            tok_s.at[kind - 1, part], tok_r.at[kind - 1, part], on_ring(way),
        )

    def tok_forward(part):
        block = 2 * core + part
        return remote(
            toks.at[1, block], toks.at[3, block],
            tok_s.at[2, part], tok_r.at[2, part], on_ring(1 if part == 0 else -1),
        )

    def tok_partner(kind, part):
        block = 2 * core + part
        return remote(
            toks.at[kind, block], toks.at[kind, block], one.at[0], tokp_r.at[kind - 1], partner
        )

    def tok_arrival(kind, part):
        block = 2 * core + part
        return remote(
            toks.at[kind, block], toks.at[kind, block],
            tok_s.at[kind - 1, part], tok_r.at[kind - 1, part], partner,
        )

    def tok_partner_arrival(kind):
        blocks = pl.ds(2 * (1 - core), 2)
        return remote(
            toks.at[kind, blocks], toks.at[kind, blocks], one.at[0], tokp_r.at[kind - 1], partner
        )

    def w_own(way, part):
        kind = kind_of(way, part)
        return remote(
            wts.at[0, part], wts.at[kind, part],
            w_s.at[kind - 1, part], w_r.at[kind - 1, part], along_x(way % 4),
        )

    def w_forward(part):
        return remote(
            wts.at[1, part], wts.at[3, part],
            w_s.at[2, part], w_r.at[2, part], along_x(1 if part == 0 else 3),
        )

    def w_arrival(kind, part):
        return remote(
            wts.at[kind, part], wts.at[kind, part],
            w_s.at[kind - 1, part], w_r.at[kind - 1, part], along_x(1),
        )

    def relay_copy(step, part):
        return remote(
            parts.at[step, (y + 2) % 4, part], relay.at[step, part],
            one.at[1], r1_r.at[step % 4, part], along_y(1 if part == 0 else 3),
        )

    def sum_copy(step, part):
        way = 1 if part == 0 else 3
        return remote(
            parts.at[step, (y + way) % 4], arrived.at[step, part],
            one.at[2], r2_r.at[step % 4, part], along_y(way),
        )

    def final_copy(step, part):
        rows, columns = unit_of(step)
        chunk = (x + places_on(columns, part)) % 4
        return remote(
            sums.at[step, part], final.at[z, chunk, part],
            one.at[3], fin_r.at[z], along_z(places_on(rows, y % 2)),
        )

    def final_arrival(place):
        return remote(final.at[place], final.at[place], one.at[3], fin_r.at[place], along_z(1))

    def index_x(step):
        return remote(idx_all.at[z, x], idx_all.at[z, x], one.at[4], one.at[5], along_x(step))

    def index_z(step):
        return remote(idx_all.at[z], idx_all.at[z], one.at[6], one.at[7], along_z(step))

    index_x_three = remote(
        idx_all.at[0, pl.ds(0, 3)], idx_all.at[0, pl.ds(0, 3)], one.at[4], one.at[5], along_x(1)
    )
    index_z_three = remote(
        idx_all.at[pl.ds(0, 3)], idx_all.at[pl.ds(0, 3)], one.at[6], one.at[7], along_z(1)
    )

    def up_columns(step):
        return pl.ds(pl.multiple_of((x + step) % 4 * SLICE, SLICE), SLICE)

    def up_near(step):
        return remote(up.at[:, :, up_columns(step)], spread.at[x], one.at[8], one.at[9], along_x(step))

    def up_cross(part):
        return remote(
            up.at[pl.ds(2 * part, 2), :, up_columns(2)], transit.at[part],
            one.at[8], one.at[10], along_x(1 if part == 0 else 3),
        )

    def up_relay(part):
        step = 1 if part == 0 else 3
        place = (x + 4 - step) % 4
        return remote(
            transit.at[part], spread.at[place, pl.ds(2 * part, 2)],
            one.at[11], one.at[9], along_x(step),
        )

    up_three = remote(spread.at[pl.ds(0, 3)], spread.at[pl.ds(0, 3)], one.at[8], one.at[9], along_x(1))
    up_transit = remote(transit, transit, one.at[11], one.at[10], along_x(1))

    mate = 1 - 2 * (z % 2)
    far = 3 - 2 * z

    def up_pair(part):
        chunk = z + mate if part == 0 else 3 - (z + mate)
        return remote(
            picked.at[chunk], zpicks.at[part], one.at[12], u2_r.at[part], along_z(mate + 4)
        )

    def up_far():
        return remote(picked.at[3 - z], zpicks.at[2], one.at[12], u2_r.at[2], along_z(far + 4))

    def up_last(step):
        return remote(
            chosen.at[(x + step) % 4], upfin.at[x], one.at[13], one.at[14], along_x(step)
        )

    def shrink_copy(step):
        return remote(
            shr.at[(y + step) % 4], shr_in.at[step - 1], one.at[15], one.at[16], along_y(step)
        )

    up_last_three = remote(
        chosen.at[pl.ds(0, 3)], upfin.at[pl.ds(0, 3)], one.at[13], one.at[14], along_x(1)
    )
    shrink_three = remote(shr_in, shr_in, one.at[15], one.at[16], along_y(1))

    loads = [
        pltpu.make_async_copy(idx_hbm, idx_ref, local_sem.at[4]),
        pltpu.make_async_copy(tok_hbm, toks.at[0], local_sem.at[0]),
        pltpu.make_async_copy(wt_hbm, wts.at[0], local_sem.at[1]),
        pltpu.make_async_copy(down_hbm, down, local_sem.at[2]),
        pltpu.make_async_copy(up_hbm, up, local_sem.at[3]),
        pltpu.make_async_copy(live_hbm, live_ref, local_sem.at[5]),
    ]
    for load in loads:
        load.start()
    barrier = pltpu.get_barrier_semaphore()
    peers = [along_x(n) for n in (1, 2, 3)] + [along_y(n) for n in (1, 2, 3)]
    peers += [along_z(n) for n in (1, 2, 3)] + [on_ring(1), on_ring(-1), partner]
    for peer in peers:
        pl.semaphore_signal(barrier, inc=1, device_id=peer, device_id_type=pl.DeviceIdType.MESH)

    loads[0].wait()
    lane = lax.broadcasted_iota(jnp.int32, (1, 128), 1)
    row = jnp.zeros((1, 128), jnp.int32)
    for block in range(4):
        row = jnp.where(lane == block, idx_ref[block], row)
    idx_all[z, x] = row
    loads[1].wait()
    loads[2].wait()
    pl.semaphore_wait(barrier, len(peers))

    for n in (1, 2, 3):
        index_x(n).start()
    for way in (1, -1):
        w_own(way, 0 if way > 0 else 1).start()
        tok_own(way, 0 if way > 0 else 1).start()
    for way in (1, -1):
        tok_own(way, 1 if way > 0 else 0).start()

    to_scalars = pltpu.make_async_copy(idx_all, idx_s, local_sem.at[0])
    own_columns = pltpu.make_async_copy(up.at[:, :, up_columns(0)], spread.at[x], local_sem.at[1])

    def step_body(step, carry):
        @pl.when((step >= LAG_RELAY) & (step < UNITS + LAG_RELAY))
        def _():
            done = step - LAG_RELAY
            for part in (0, 1):
                to = (y + (1 if part == 0 else 3)) % 4
                relay_copy(done, part).wait_recv()
                added = parts[done, to, part].astype(F32) + relay[done, part].astype(F32)
                parts[done, to, part] = added.astype(BF)

        @pl.when((step >= LAG_RELAY) & (step < UNITS + LAG_RELAY))
        def _():
            for part in (0, 1):
                sum_copy(step - LAG_RELAY, part).start()

        @pl.when(step >= LAG_SUM)
        def _():
            done = step - LAG_SUM
            rows, columns = unit_of(done)
            for part in (0, 1):
                sum_copy(done, part).wait_recv()
            total = parts[done, y].astype(F32) + arrived[done, 0].astype(F32)
            total = (total + arrived[done, 1].astype(F32)).astype(BF)

            @pl.when(rows == 0)
            def _():
                for part in (0, 1):
                    final[z, (x + places_on(columns, part)) % 4, part] = total[part]

            @pl.when(rows > 0)
            def _():
                sums[done] = total
                for part in (0, 1):
                    final_copy(done, part).start()

        @pl.when(step == 1)
        def _():
            loads[3].wait()
            for block in range(4):
                chosen_down = down[idx_ref[block]]
                shr[block] = lax.dot_general(
                    chosen_down, toks[0, block], LAST, preferred_element_type=F32
                )
            for n in (1, 2, 3):
                shrink_copy(n).start()
            index_x_three.wait_recv()
            for n in (1, 2, 3):
                index_z(n).start()

        @pl.when(step == 1)
        def _():
            loads[4].wait()
            for way in (1, -1):
                part = 0 if way > 0 else 1
                w_own(way, part).wait_send()
                up_near(way % 4).start()
                up_cross(part).start()
            for part in (0, 1):
                tok_arrival(1, part).wait_recv()
                tok_partner(1, part).start()
            for part in (0, 1):
                w_arrival(1, part).wait_recv()

        @pl.when(step == 2)
        def _():
            up_three.wait_send()
            for way in (1, -1):
                part = 0 if way > 0 else 1
                w_own(way, 1 - part).start()
            tok_partner_arrival(1).wait_recv()

        @pl.when(step == 3)
        def _():
            for way in (1, -1):
                part = 0 if way > 0 else 1
                tok_own(way, 1 - part).wait_send()
                tok_forward(part).start()

        @pl.when(step == 4)
        def _():
            tok_partner_arrival(2).wait_recv()

        @pl.when(step == 6)
        def _():
            for part in (0, 1):
                w_arrival(2, part).wait_recv()
                w_forward(part).start()
            for part in (0, 1):
                tok_arrival(3, part).wait_recv()
                tok_partner(3, part).start()

        @pl.when(step == 7)
        def _():
            tok_partner_arrival(3).wait_recv()

        @pl.when(step == 10)
        def _():
            for part in (0, 1):
                w_arrival(3, part).wait_recv()

        @pl.when(step < UNITS)
        def _():
            s, t = unit_of(step)
            result = lax.dot_general(
                wts[t].reshape(COLS, WIDTH), toks[s].reshape(4 * BLOCK, WIDTH), LAST,
                preferred_element_type=F32,
            ).astype(BF)
            for block in range(4):
                tile = result[:, block * BLOCK : (block + 1) * BLOCK]
                parts[step, block] = tile.reshape(2, HALF, BLOCK)

        @pl.when(step < UNITS)
        def _():
            for part in (0, 1):
                relay_copy(step, part).start()

        @pl.when(step == 3)
        def _():
            for part in (0, 1):
                tok_arrival(2, part).wait_recv()
                tok_partner(2, part).start()
            up_transit.wait_recv()
            for part in (0, 1):
                up_relay(part).start()
            own_columns.start()

        @pl.when(step == PICK_STEP)
        def _():
            index_z_three.wait_recv()
            to_scalars.start()
            up_three.wait_recv()
            to_scalars.wait()
            own_columns.wait()
            for to_z in range(4):
                for to_x in range(4):
                    local = idx_s[to_z, to_x, 0, y] - 16 * z
                    owned = jnp.where((local >= 0) & (local < 16), 1.0, 0.0).astype(F32)
                    kept = jnp.clip(local, 0, 15)
                    factor = spread[kept // 4, kept % 4].astype(F32) * owned
                    picked[to_z, to_x] = factor.astype(BF)
            for part in (1, 0):
                up_pair(part).start()

        @pl.when(step == PAIR_STEP)
        def _():
            up_pair(1).wait_recv()
            for to_x in range(4):
                picked[3 - z, to_x] = picked[3 - z, to_x] + zpicks[1, to_x]
            up_far().start()

        @pl.when(step == FAR_STEP)
        def _():
            up_pair(0).wait_recv()
            up_far().wait_recv()
            for to_x in range(4):
                chosen[to_x] = (picked[z, to_x] + zpicks[0, to_x]) + zpicks[2, to_x]
            for n in (1, 2, 3):
                up_last(n).start()
            upfin[x] = chosen[x]

        return carry

    lax.fori_loop(0, UNITS + LAG_SUM, step_body, 0)

    def finish_sends():
        index_x_three.wait_send()
        index_z_three.wait_send()
        shrink_three.wait_send()
        up_transit.wait_send()
        remote(zpicks, zpicks, one.at[12], u2_r.at[0], partner).wait_send()
        up_last_three.wait_send()
        for part in (0, 1):
            way = 1 if part == 0 else -1
            w_own(way, 1 - part).wait_send()
            tok_own(way, part).wait_send()
            w_forward(part).wait_send()
            tok_forward(part).wait_send()
        passed = toks.at[pl.ds(1, 3), pl.ds(0, 2)]
        remote(passed, passed, one.at[0], tokp_r.at[0], partner).wait_send()
        remote(relay, relay, one.at[1], r1_r.at[0, 0], partner).wait_send()
        remote(arrived, arrived, one.at[2], r2_r.at[0, 0], partner).wait_send()

    shrink_three.wait_recv()
    low = (shr[y] + shr_in[0] + (shr_in[1] + shr_in[2])).astype(BF)
    same = lax.broadcasted_iota(jnp.int32, (BLOCK, BLOCK), 0) == lax.broadcasted_iota(
        jnp.int32, (BLOCK, BLOCK), 1
    )
    eye = jnp.where(same, 1.0, 0.0).astype(BF)
    turned = lax.dot_general(eye, low, LAST, preferred_element_type=F32)
    doubled = (2.0 * turned).astype(BF)
    loads[5].wait()
    live = lax.broadcasted_iota(jnp.int32, (BLOCK, 1), 0) < live_ref[y]
    up_last_three.wait_recv()

    for n in (0, 1, 3, 2):
        place = (z + n) % 4
        if n:
            final_arrival(place).wait_recv()
        base = lax.dot_general(
            eye, final[place].reshape(SLICE, BLOCK), LAST, preferred_element_type=F32
        )
        extra = jnp.dot(doubled, upfin[place], preferred_element_type=F32)
        columns = pl.ds(pl.multiple_of(place * SLICE, SLICE), SLICE)
        out_ref[:, columns] = jnp.where(live, base + extra, 0.0).astype(BF)
        if n == 0:
            finish_sends()
    gone = sums.at[pl.ds(*AWAY)]
    remote(gone, gone, one.at[3], fin_r.at[z], partner).wait_send()


def body(tokens, base_up_weight, adapter_down_weight, adapter_up_weight, block_adapter_index, request_rows):
    dma = pltpu.SemaphoreType.DMA
    half_tile = (2, HALF, BLOCK)
    any_space = pl.BlockSpec(memory_space=pl.ANY)
    return pl.pallas_call(
        kernel,
        out_shape=pltpu.VMEM((BLOCK, 4 * SLICE), BF),
        in_specs=[any_space] * 6,
        out_specs=pl.BlockSpec(memory_space=pltpu.VMEM),
        scratch_shapes=[
            pltpu.VMEM((4, 4, BLOCK, WIDTH), BF),
            pltpu.VMEM((4, 2, HALF, WIDTH), BF),
            pltpu.VMEM((CATALOG, RANK, WIDTH), BF),
            pltpu.VMEM((4, RANK, 4 * SLICE), BF),
            pltpu.VMEM((UNITS, 4, *half_tile), BF),
            pltpu.VMEM((UNITS, *half_tile), BF),
            pltpu.VMEM((UNITS, 2, *half_tile), BF),
            pltpu.VMEM((UNITS, *half_tile), BF),
            pltpu.VMEM((4, 4, *half_tile), BF),
            pltpu.VMEM((4, RANK, SLICE), BF),
            pltpu.SMEM((4,), jnp.int32),
            pltpu.SMEM((4,), jnp.int32),
            pltpu.VMEM((4, 4, 1, 128), jnp.int32),
            pltpu.SMEM((4, 4, 1, 128), jnp.int32),
            pltpu.VMEM((4, 4, RANK, SLICE), BF),
            pltpu.VMEM((2, 2, RANK, SLICE), BF),
            pltpu.VMEM((4, 4, RANK, SLICE), BF),
            pltpu.VMEM((3, 4, RANK, SLICE), BF),
            pltpu.VMEM((4, RANK, SLICE), BF),
            pltpu.VMEM((4, RANK, BLOCK), F32),
            pltpu.VMEM((3, RANK, BLOCK), F32),
            dma((6,)), dma((17,)),
            dma((3, 2)), dma((3, 2)), dma((3,)), dma((3, 2)), dma((3, 2)),
            dma((4, 2)), dma((4, 2)), dma((4,)), dma((3,)),
        ],
        compiler_params=pltpu.CompilerParams(
            collective_id=0, has_side_effects=True, vmem_limit_bytes=60000000
        ),
    )(
        block_adapter_index,
        request_rows,
        tokens.reshape(4, BLOCK, WIDTH),
        base_up_weight.T.reshape(2, HALF, WIDTH),
        adapter_down_weight,
        adapter_up_weight,
    )


def solution(mesh):
    in_specs = (
        P("gx", "gy"),
        P("gy", ("gz", "gx")),
        P(None, None, "gy"),
        P("gx", None, "gz"),
        P("gx"),
        P("gx"),
    )
    out_specs = P(("gx", "gy"), "gz")
    return jax.shard_map(body, mesh=mesh, in_specs=in_specs, out_specs=out_specs, check_vma=False)
```

```python
import functools

import jax
import jax.numpy as jnp
from jax import lax
from jax.experimental import pallas as pl
from jax.experimental.pallas import tpu as pltpu
from jax.sharding import PartitionSpec as P

BLOCK = 128
RANK = 16
CATALOG = 64
WIDTH = 1152
COLS = 288
HALF = COLS // 2
SLICE = 4 * COLS
UNITS = 16
LAG_RELAY = 2
LAG_SUM = 4
PICK_STEP = 5
PAIR_STEP = 7
FAR_STEP = 18
AWAY = (2, 12)
BF = jnp.bfloat16
F32 = jnp.float32
LAST = (((1,), (1,)), ((), ()))


ORDER = (
    (0, 0), (0, 1), (1, 0), (1, 1), (3, 0), (3, 1), (1, 2), (3, 2),
    (2, 0), (2, 1), (3, 3), (1, 3), (2, 2), (2, 3), (0, 2), (0, 3),
)


def staircase(step, column):
    rises = [(at, ORDER[at][column] - ORDER[at - 1][column]) for at in range(1, UNITS)]
    return sum(rise * ((step + 16 - at) // 16) for at, rise in rises if rise)


def unit_of(step):
    return staircase(step, 0), staircase(step, 1)


def places_on(kind, part):
    three = kind // 3
    two = kind // 2 - three
    one = kind - 2 * (kind // 2) - three
    return one * (3 - 2 * part) + two * (1 + 2 * part) + 2 * three


def kernel(
    idx_hbm, live_hbm, tok_hbm, wt_hbm, down_hbm, up_hbm, out_ref,
    toks, wts, down, up, parts, relay, arrived, sums, final, upfin,
    idx_ref, live_ref, idx_all, idx_s, spread, transit, picked, zpicks, chosen, shr, shr_in,
    local_sem, one, tok_s, tok_r, tokp_r, w_s, w_r, r1_r, r2_r, fin_r, u2_r,
):
    gx = lax.axis_index("gx")
    y = lax.axis_index("gy")
    gz = lax.axis_index("gz")
    z, x = gx // 4, gx % 4
    zh, core = gz // 2, gz % 2
    ring = zh * 4 + z

    def along_x(step):
        return (z * 4 + (x + step) % 4, y, gz)

    def along_y(step):
        return (gx, (y + step) % 4, gz)

    def along_z(step):
        return (((z + step) % 4) * 4 + x, y, gz)

    def on_ring(step):
        place = (ring + step) % 8
        return ((place % 4) * 4 + x, y, (place // 4) * 2 + core)

    partner = (gx, y, zh * 2 + 1 - core)

    def remote(src, dst, send, recv, to):
        return pltpu.make_async_remote_copy(
            src_ref=src, dst_ref=dst, send_sem=send, recv_sem=recv,
            device_id=to, device_id_type=pl.DeviceIdType.MESH,
        )

    def kind_of(way, part):
        return 1 if (way > 0) == (part == 0) else 2

    def tok_own(way, part):
        kind, block = kind_of(way, part), 2 * core + part
        return remote(
            toks.at[0, block], toks.at[kind, block],
            tok_s.at[kind - 1], tok_r.at[kind - 1], on_ring(way),
        )

    def tok_forward(part):
        block = 2 * core + part
        return remote(
            toks.at[1, block], toks.at[3, block],
            tok_s.at[2], tok_r.at[2], on_ring(1 if part == 0 else -1),
        )

    def tok_partner(kind, part):
        block = 2 * core + part
        return remote(
            toks.at[kind, block], toks.at[kind, block], one.at[0], tokp_r.at[kind - 1], partner
        )

    def tok_pair(kind):
        blocks = pl.ds(2 * core, 2)
        return remote(
            toks.at[kind, blocks], toks.at[kind, blocks], tok_s.at[kind - 1], tok_r.at[kind - 1], partner
        )

    def tok_partner_arrival(kind):
        blocks = pl.ds(2 * (1 - core), 2)
        return remote(
            toks.at[kind, blocks], toks.at[kind, blocks], one.at[0], tokp_r.at[kind - 1], partner
        )

    def w_own(way, part):
        kind = kind_of(way, part)
        return remote(
            wts.at[0, part], wts.at[kind, part],
            w_s.at[kind - 1], w_r.at[kind - 1], along_x(way % 4),
        )

    def w_forward(part):
        return remote(
            wts.at[1, part], wts.at[3, part],
            w_s.at[2], w_r.at[2], along_x(1 if part == 0 else 3),
        )

    def w_pair(kind):
        return remote(wts.at[kind], wts.at[kind], w_s.at[kind - 1], w_r.at[kind - 1], along_x(1))

    def relay_copy(step, part):
        return remote(
            parts.at[step, (y + 2) % 4, part], relay.at[step, part],
            one.at[1], r1_r.at[step % 4, part], along_y(1 if part == 0 else 3),
        )

    def sum_copy(step, part):
        way = 1 if part == 0 else 3
        return remote(
            parts.at[step, (y + way) % 4], arrived.at[step, part],
            one.at[2], r2_r.at[step % 4, part], along_y(way),
        )

    def final_copy(step, part):
        rows, columns = unit_of(step)
        chunk = (x + places_on(columns, part)) % 4
        return remote(
            sums.at[step, part], final.at[z, chunk, part],
            one.at[3], fin_r.at[z], along_z(places_on(rows, y % 2)),
        )

    def final_arrival(place):
        return remote(final.at[place], final.at[place], one.at[3], fin_r.at[place], along_z(1))

    def index_x(step):
        return remote(idx_all.at[z, x], idx_all.at[z, x], one.at[4], one.at[5], along_x(step))

    def index_z(step):
        return remote(idx_all.at[z], idx_all.at[z], one.at[6], one.at[7], along_z(step))

    index_x_three = remote(
        idx_all.at[0, pl.ds(0, 3)], idx_all.at[0, pl.ds(0, 3)], one.at[4], one.at[5], along_x(1)
    )
    index_z_three = remote(
        idx_all.at[pl.ds(0, 3)], idx_all.at[pl.ds(0, 3)], one.at[6], one.at[7], along_z(1)
    )

    def up_columns(step):
        return pl.ds(pl.multiple_of((x + step) % 4 * SLICE, SLICE), SLICE)

    def up_near(step):
        return remote(up.at[:, :, up_columns(step)], spread.at[x], one.at[8], one.at[9], along_x(step))

    def up_cross(part):
        return remote(
            up.at[pl.ds(2 * part, 2), :, up_columns(2)], transit.at[part],
            one.at[8], one.at[10], along_x(1 if part == 0 else 3),
        )

    def up_relay(part):
        step = 1 if part == 0 else 3
        place = (x + 4 - step) % 4
        return remote(
            transit.at[part], spread.at[place, pl.ds(2 * part, 2)],
            one.at[11], one.at[9], along_x(step),
        )

    up_three = remote(spread.at[pl.ds(0, 3)], spread.at[pl.ds(0, 3)], one.at[8], one.at[9], along_x(1))
    up_transit = remote(transit, transit, one.at[11], one.at[10], along_x(1))

    mate = 1 - 2 * (z % 2)
    far = 3 - 2 * z

    def up_pair(part):
        chunk = z + mate if part == 0 else 3 - (z + mate)
        return remote(
            picked.at[chunk], zpicks.at[part], one.at[12], u2_r.at[part], along_z(mate + 4)
        )

    def up_far():
        return remote(picked.at[3 - z], zpicks.at[2], one.at[12], u2_r.at[2], along_z(far + 4))

    def up_last(step):
        return remote(
            chosen.at[(x + step) % 4], upfin.at[x], one.at[13], one.at[14], along_x(step)
        )

    def shrink_copy(step):
        return remote(
            shr.at[(y + step) % 4], shr_in.at[step - 1], one.at[15], one.at[16], along_y(step)
        )

    up_last_three = remote(
        chosen.at[pl.ds(0, 3)], upfin.at[pl.ds(0, 3)], one.at[13], one.at[14], along_x(1)
    )
    shrink_three = remote(shr_in, shr_in, one.at[15], one.at[16], along_y(1))

    loads = [
        pltpu.make_async_copy(idx_hbm, idx_ref, local_sem.at[4]),
        pltpu.make_async_copy(tok_hbm, toks.at[0], local_sem.at[0]),
        pltpu.make_async_copy(wt_hbm, wts.at[0], local_sem.at[1]),
        pltpu.make_async_copy(down_hbm, down, local_sem.at[2]),
        pltpu.make_async_copy(up_hbm, up, local_sem.at[3]),
        pltpu.make_async_copy(live_hbm, live_ref, local_sem.at[5]),
    ]
    for load in loads:
        load.start()
    barrier = pltpu.get_barrier_semaphore()
    peers = [along_x(n) for n in (1, 2, 3)] + [along_y(n) for n in (1, 2, 3)]
    peers += [along_z(n) for n in (1, 2, 3)] + [on_ring(1), on_ring(-1), partner]
    for peer in peers:
        pl.semaphore_signal(barrier, inc=1, device_id=peer, device_id_type=pl.DeviceIdType.MESH)

    loads[0].wait()
    lane = lax.broadcasted_iota(jnp.int32, (1, 128), 1)
    row = jnp.zeros((1, 128), jnp.int32)
    for block in range(4):
        row = jnp.where(lane == block, idx_ref[block], row)
    idx_all[z, x] = row
    loads[1].wait()
    loads[2].wait()
    pl.semaphore_wait(barrier, len(peers))

    for way in (1, -1):
        tok_own(way, 0 if way > 0 else 1).start()
    for n in (1, 2, 3):
        index_x(n).start()
    for way in (1, -1):
        w_own(way, 0 if way > 0 else 1).start()

    to_scalars = pltpu.make_async_copy(idx_all, idx_s, local_sem.at[0])
    own_columns = pltpu.make_async_copy(up.at[:, :, up_columns(0)], spread.at[x], local_sem.at[1])

    def step_body(step, carry):
        @pl.when(step >= LAG_SUM)
        def _():
            done = step - LAG_SUM
            rows, columns = unit_of(done)
            for part in (0, 1):
                sum_copy(done, part).wait_recv()
            total = parts[done, y].astype(F32) + arrived[done, 0].astype(F32)
            total = (total + arrived[done, 1].astype(F32)).astype(BF)

            @pl.when(rows == 0)
            def _():
                for part in (0, 1):
                    final[z, (x + places_on(columns, part)) % 4, part] = total[part]

            @pl.when(rows > 0)
            def _():
                sums[done] = total
                for part in (0, 1):
                    final_copy(done, part).start()

        @pl.when((step >= LAG_RELAY) & (step < UNITS + LAG_RELAY))
        def _():
            done = step - LAG_RELAY
            for part in (0, 1):
                to = (y + (1 if part == 0 else 3)) % 4
                relay_copy(done, part).wait_recv()
                added = parts[done, to, part].astype(F32) + relay[done, part].astype(F32)
                parts[done, to, part] = added.astype(BF)

        @pl.when((step >= LAG_RELAY) & (step < UNITS + LAG_RELAY))
        def _():
            for part in (0, 1):
                sum_copy(step - LAG_RELAY, part).start()

        @pl.when(step == 1)
        def _():
            loads[3].wait()
            for block in range(4):
                chosen_down = down[idx_ref[block]]
                shr[block] = lax.dot_general(
                    chosen_down, toks[0, block], LAST, preferred_element_type=F32
                )
            for n in (1, 2, 3):
                shrink_copy(n).start()
            index_x_three.wait_recv()
            for n in (1, 2, 3):
                index_z(n).start()

        @pl.when(step == 1)
        def _():
            loads[4].wait()
            w_pair(1).wait_send()
            for way in (1, -1):
                part = 0 if way > 0 else 1
                up_near(way % 4).start()
                up_cross(part).start()
            tok_pair(1).wait_recv()
            for part in (0, 1):
                tok_forward(part).start()
                tok_partner(1, part).start()
            w_pair(1).wait_recv()

        @pl.when(step == 2)
        def _():
            up_three.wait_send()
            for way in (1, -1):
                part = 0 if way > 0 else 1
                w_own(way, 1 - part).start()
            tok_partner_arrival(1).wait_recv()

        @pl.when(step == 3)
        def _():
            tok_pair(3).wait_send()
            for way in (1, -1):
                tok_own(way, 1 if way > 0 else 0).start()

        @pl.when(step == 4)
        def _():
            tok_partner_arrival(3).wait_recv()

        @pl.when(step == 6)
        def _():
            w_pair(2).wait_recv()
            for part in (0, 1):
                w_forward(part).start()
            tok_pair(2).wait_recv()
            for part in (0, 1):
                tok_partner(2, part).start()

        @pl.when(step == 8)
        def _():
            tok_partner_arrival(2).wait_recv()

        @pl.when(step == 10)
        def _():
            w_pair(3).wait_recv()

        @pl.when(step < UNITS)
        def _():
            s, t = unit_of(step)
            result = lax.dot_general(
                wts[t].reshape(COLS, WIDTH), toks[s].reshape(4 * BLOCK, WIDTH), LAST,
                preferred_element_type=F32,
            ).astype(BF)
            for block in range(4):
                tile = result[:, block * BLOCK : (block + 1) * BLOCK]
                parts[step, block] = tile.reshape(2, HALF, BLOCK)

        @pl.when(step < UNITS)
        def _():
            for part in (0, 1):
                relay_copy(step, part).start()

        @pl.when(step == 3)
        def _():
            tok_pair(3).wait_recv()
            for part in (0, 1):
                tok_partner(3, part).start()
            up_transit.wait_recv()
            for part in (0, 1):
                up_relay(part).start()
            own_columns.start()

        @pl.when(step == PICK_STEP - 1)
        def _():
            index_z_three.wait_recv()
            to_scalars.start()

        @pl.when(step == PICK_STEP)
        def _():
            up_three.wait_recv()
            to_scalars.wait()
            own_columns.wait()
            for to_z in range(4):
                for to_x in range(4):
                    local = idx_s[to_z, to_x, 0, y] - 16 * z
                    owned = jnp.where((local >= 0) & (local < 16), 1.0, 0.0).astype(F32)
                    kept = jnp.clip(local, 0, 15)
                    factor = spread[kept // 4, kept % 4].astype(F32) * owned
                    picked[to_z, to_x] = factor.astype(BF)
            for part in (1, 0):
                up_pair(part).start()

        @pl.when(step == PAIR_STEP)
        def _():
            up_pair(1).wait_recv()
            for to_x in range(4):
                picked[3 - z, to_x] = picked[3 - z, to_x] + zpicks[1, to_x]
            up_far().start()

        @pl.when(step == FAR_STEP)
        def _():
            up_pair(0).wait_recv()
            up_far().wait_recv()
            for to_x in range(4):
                chosen[to_x] = (picked[z, to_x] + zpicks[0, to_x]) + zpicks[2, to_x]
            for n in (1, 2, 3):
                up_last(n).start()
            upfin[x] = chosen[x]

        return carry

    lax.fori_loop(0, UNITS + LAG_SUM, step_body, 0)

    def finish_sends():
        index_x_three.wait_send()
        index_z_three.wait_send()
        shrink_three.wait_send()
        up_transit.wait_send()
        remote(zpicks, zpicks, one.at[12], u2_r.at[0], partner).wait_send()
        up_last_three.wait_send()
        tok_pair(1).wait_send()
        tok_pair(2).wait_send()
        w_pair(2).wait_send()
        w_pair(3).wait_send()
        passed = toks.at[pl.ds(1, 3), pl.ds(0, 2)]
        remote(passed, passed, one.at[0], tokp_r.at[0], partner).wait_send()
        remote(relay, relay, one.at[1], r1_r.at[0, 0], partner).wait_send()
        remote(arrived, arrived, one.at[2], r2_r.at[0, 0], partner).wait_send()

    shrink_three.wait_recv()
    low = (shr[y] + shr_in[0] + (shr_in[1] + shr_in[2])).astype(BF)
    same = lax.broadcasted_iota(jnp.int32, (BLOCK, BLOCK), 0) == lax.broadcasted_iota(
        jnp.int32, (BLOCK, BLOCK), 1
    )
    eye = jnp.where(same, 1.0, 0.0).astype(BF)
    turned = lax.dot_general(eye, low, LAST, preferred_element_type=F32)
    doubled = (2.0 * turned).astype(BF)
    loads[5].wait()
    live = lax.broadcasted_iota(jnp.int32, (BLOCK, 1), 0) < live_ref[y]
    up_last_three.wait_recv()

    for n in (0, 1, 3, 2):
        place = (z + n) % 4
        if n:
            final_arrival(place).wait_recv()
        base = lax.dot_general(
            eye, final[place].reshape(SLICE, BLOCK), LAST, preferred_element_type=F32
        )
        extra = jnp.dot(doubled, upfin[place], preferred_element_type=F32)
        columns = pl.ds(pl.multiple_of(place * SLICE, SLICE), SLICE)
        out_ref[:, columns] = jnp.where(live, base + extra, 0.0).astype(BF)
        if n == 0:
            finish_sends()
    gone = sums.at[pl.ds(*AWAY)]
    remote(gone, gone, one.at[3], fin_r.at[z], partner).wait_send()


def body(tokens, base_up_weight, adapter_down_weight, adapter_up_weight, block_adapter_index, request_rows):
    dma = pltpu.SemaphoreType.DMA
    half_tile = (2, HALF, BLOCK)
    any_space = pl.BlockSpec(memory_space=pl.ANY)
    return pl.pallas_call(
        kernel,
        out_shape=pltpu.VMEM((BLOCK, 4 * SLICE), BF),
        in_specs=[any_space] * 6,
        out_specs=pl.BlockSpec(memory_space=pltpu.VMEM),
        scratch_shapes=[
            pltpu.VMEM((4, 4, BLOCK, WIDTH), BF),
            pltpu.VMEM((4, 2, HALF, WIDTH), BF),
            pltpu.VMEM((CATALOG, RANK, WIDTH), BF),
            pltpu.VMEM((4, RANK, 4 * SLICE), BF),
            pltpu.VMEM((UNITS, 4, *half_tile), BF),
            pltpu.VMEM((UNITS, *half_tile), BF),
            pltpu.VMEM((UNITS, 2, *half_tile), BF),
            pltpu.VMEM((UNITS, *half_tile), BF),
            pltpu.VMEM((4, 4, *half_tile), BF),
            pltpu.VMEM((4, RANK, SLICE), BF),
            pltpu.SMEM((4,), jnp.int32),
            pltpu.SMEM((4,), jnp.int32),
            pltpu.VMEM((4, 4, 1, 128), jnp.int32),
            pltpu.SMEM((4, 4, 1, 128), jnp.int32),
            pltpu.VMEM((4, 4, RANK, SLICE), BF),
            pltpu.VMEM((2, 2, RANK, SLICE), BF),
            pltpu.VMEM((4, 4, RANK, SLICE), BF),
            pltpu.VMEM((3, 4, RANK, SLICE), BF),
            pltpu.VMEM((4, RANK, SLICE), BF),
            pltpu.VMEM((4, RANK, BLOCK), F32),
            pltpu.VMEM((3, RANK, BLOCK), F32),
            dma((6,)), dma((17,)),
            dma((3,)), dma((3,)), dma((3,)), dma((3,)), dma((3,)),
            dma((4, 2)), dma((4, 2)), dma((4,)), dma((3,)),
        ],
        compiler_params=pltpu.CompilerParams(
            collective_id=0, has_side_effects=True, vmem_limit_bytes=60000000
        ),
    )(
        block_adapter_index,
        request_rows,
        tokens.reshape(4, BLOCK, WIDTH),
        base_up_weight.T.reshape(2, HALF, WIDTH),
        adapter_down_weight,
        adapter_up_weight,
    )


def solution(mesh):
    in_specs = (
        P("gx", "gy"),
        P("gy", ("gz", "gx")),
        P(None, None, "gy"),
        P("gx", None, "gz"),
        P("gx"),
        P("gx"),
    )
    out_specs = P(("gx", "gy"), "gz")
    return jax.shard_map(body, mesh=mesh, in_specs=in_specs, out_specs=out_specs, check_vma=False)
```

```python
import functools

import jax
import jax.numpy as jnp
from jax import lax
from jax.experimental import pallas as pl
from jax.experimental.pallas import tpu as pltpu
from jax.sharding import PartitionSpec as P

BLOCK = 128
RANK = 16
CATALOG = 64
WIDTH = 1152
COLS = 288
HALF = COLS // 2
SLICE = 4 * COLS
UNITS = 16
LAG_RELAY = 2
LAG_SUM = 4
PICK_STEP = 5
PAIR_STEP = 7
FAR_STEP = 16
AWAY = (2, 12)
BF = jnp.bfloat16
F32 = jnp.float32
LAST = (((1,), (1,)), ((), ()))


ORDER = (
    (0, 0), (0, 1), (1, 0), (1, 1), (3, 0), (3, 1), (1, 2), (3, 2),
    (2, 0), (2, 1), (3, 3), (1, 3), (2, 2), (2, 3), (0, 2), (0, 3),
)


def staircase(step, column):
    rises = [(at, ORDER[at][column] - ORDER[at - 1][column]) for at in range(1, UNITS)]
    return sum(rise * ((step + 16 - at) // 16) for at, rise in rises if rise)


def unit_of(step):
    return staircase(step, 0), staircase(step, 1)


def places_on(kind, part):
    three = kind // 3
    two = kind // 2 - three
    one = kind - 2 * (kind // 2) - three
    return one * (3 - 2 * part) + two * (1 + 2 * part) + 2 * three


def kernel(
    idx_hbm, live_hbm, tok_hbm, wt_hbm, down_hbm, up_hbm, out_ref,
    toks, wts, down, up, parts, relay, arrived, sums, final, upfin,
    idx_ref, live_ref, idx_all, idx_s, spread, transit, picked, zpicks, chosen, shr, shr_in,
    local_sem, one, tok_s, tok_r, tokp_r, w_s, w_r, r1_r, r2_r, fin_r, u2_r,
):
    gx = lax.axis_index("gx")
    y = lax.axis_index("gy")
    gz = lax.axis_index("gz")
    z, x = gx // 4, gx % 4
    zh, core = gz // 2, gz % 2
    ring = zh * 4 + z

    def along_x(step):
        return (z * 4 + (x + step) % 4, y, gz)

    def along_y(step):
        return (gx, (y + step) % 4, gz)

    def along_z(step):
        return (((z + step) % 4) * 4 + x, y, gz)

    def on_ring(step):
        place = (ring + step) % 8
        return ((place % 4) * 4 + x, y, (place // 4) * 2 + core)

    partner = (gx, y, zh * 2 + 1 - core)

    def remote(src, dst, send, recv, to):
        return pltpu.make_async_remote_copy(
            src_ref=src, dst_ref=dst, send_sem=send, recv_sem=recv,
            device_id=to, device_id_type=pl.DeviceIdType.MESH,
        )

    def kind_of(way, part):
        return 1 if (way > 0) == (part == 0) else 2

    def tok_own(way, part):
        kind, block = kind_of(way, part), 2 * core + part
        return remote(
            toks.at[0, block], toks.at[kind, block],
            tok_s.at[kind - 1], tok_r.at[kind - 1], on_ring(way),
        )

    def tok_forward(part):
        block = 2 * core + part
        return remote(
            toks.at[1, block], toks.at[3, block],
            tok_s.at[2], tok_r.at[2], on_ring(1 if part == 0 else -1),
        )

    def tok_partner(kind, part):
        block = 2 * core + part
        return remote(
            toks.at[kind, block], toks.at[kind, block], one.at[0], tokp_r.at[kind - 1], partner
        )

    def tok_pair(kind):
        blocks = pl.ds(2 * core, 2)
        return remote(
            toks.at[kind, blocks], toks.at[kind, blocks], tok_s.at[kind - 1], tok_r.at[kind - 1], partner
        )

    def tok_partner_arrival(kind):
        blocks = pl.ds(2 * (1 - core), 2)
        return remote(
            toks.at[kind, blocks], toks.at[kind, blocks], one.at[0], tokp_r.at[kind - 1], partner
        )

    def w_own(way, part):
        kind = kind_of(way, part)
        return remote(
            wts.at[0, part], wts.at[kind, part],
            w_s.at[kind - 1], w_r.at[kind - 1], along_x(way % 4),
        )

    def w_forward(part):
        return remote(
            wts.at[1, part], wts.at[3, part],
            w_s.at[2], w_r.at[2], along_x(1 if part == 0 else 3),
        )

    def w_pair(kind):
        return remote(wts.at[kind], wts.at[kind], w_s.at[kind - 1], w_r.at[kind - 1], along_x(1))

    def relay_copy(step, part):
        return remote(
            parts.at[step, (y + 2) % 4, part], relay.at[step, part],
            one.at[1], r1_r.at[step % 4, part], along_y(1 if part == 0 else 3),
        )

    def sum_copy(step, part):
        way = 1 if part == 0 else 3
        return remote(
            parts.at[step, (y + way) % 4], arrived.at[step, part],
            one.at[2], r2_r.at[step % 4, part], along_y(way),
        )

    def final_copy(step, part):
        rows, columns = unit_of(step)
        chunk = (x + places_on(columns, part)) % 4
        return remote(
            sums.at[step, part], final.at[z, chunk, part],
            one.at[3], fin_r.at[z], along_z(places_on(rows, y % 2)),
        )

    def final_arrival(place):
        return remote(final.at[place], final.at[place], one.at[3], fin_r.at[place], along_z(1))

    def index_x(step):
        return remote(idx_all.at[z, x], idx_all.at[z, x], one.at[4], one.at[5], along_x(step))

    def index_z(step):
        return remote(idx_all.at[z], idx_all.at[z], one.at[6], one.at[7], along_z(step))

    index_x_three = remote(
        idx_all.at[0, pl.ds(0, 3)], idx_all.at[0, pl.ds(0, 3)], one.at[4], one.at[5], along_x(1)
    )
    index_z_three = remote(
        idx_all.at[pl.ds(0, 3)], idx_all.at[pl.ds(0, 3)], one.at[6], one.at[7], along_z(1)
    )

    def up_columns(step):
        return pl.ds(pl.multiple_of((x + step) % 4 * SLICE, SLICE), SLICE)

    def up_near(step):
        return remote(up.at[:, :, up_columns(step)], spread.at[x], one.at[8], one.at[9], along_x(step))

    def up_cross(part):
        return remote(
            up.at[pl.ds(2 * part, 2), :, up_columns(2)], transit.at[part],
            one.at[8], one.at[10], along_x(1 if part == 0 else 3),
        )

    def up_relay(part):
        step = 1 if part == 0 else 3
        place = (x + 4 - step) % 4
        return remote(
            transit.at[part], spread.at[place, pl.ds(2 * part, 2)],
            one.at[11], one.at[9], along_x(step),
        )

    up_three = remote(spread.at[pl.ds(0, 3)], spread.at[pl.ds(0, 3)], one.at[8], one.at[9], along_x(1))
    up_transit = remote(transit, transit, one.at[11], one.at[10], along_x(1))

    mate = 1 - 2 * (z % 2)
    far = 3 - 2 * z

    def up_pair(part):
        chunk = z + mate if part == 0 else 3 - (z + mate)
        return remote(
            picked.at[chunk], zpicks.at[part], one.at[12], u2_r.at[part], along_z(mate + 4)
        )

    def up_far():
        return remote(picked.at[3 - z], zpicks.at[2], one.at[12], u2_r.at[2], along_z(far + 4))

    def up_last(step):
        return remote(
            chosen.at[(x + step) % 4], upfin.at[x], one.at[13], one.at[14], along_x(step)
        )

    def shrink_copy(step):
        return remote(
            shr.at[(y + step) % 4], shr_in.at[step - 1], one.at[15], one.at[16], along_y(step)
        )

    up_last_three = remote(
        chosen.at[pl.ds(0, 3)], upfin.at[pl.ds(0, 3)], one.at[13], one.at[14], along_x(1)
    )
    shrink_three = remote(shr_in, shr_in, one.at[15], one.at[16], along_y(1))

    loads = [
        pltpu.make_async_copy(idx_hbm, idx_ref, local_sem.at[4]),
        pltpu.make_async_copy(tok_hbm, toks.at[0], local_sem.at[0]),
        pltpu.make_async_copy(wt_hbm, wts.at[0], local_sem.at[1]),
        pltpu.make_async_copy(down_hbm, down, local_sem.at[2]),
        pltpu.make_async_copy(up_hbm, up, local_sem.at[3]),
        pltpu.make_async_copy(live_hbm, live_ref, local_sem.at[5]),
    ]
    for load in loads:
        load.start()
    barrier = pltpu.get_barrier_semaphore()
    peers = [along_x(n) for n in (1, 2, 3)] + [along_y(n) for n in (1, 2, 3)]
    peers += [along_z(n) for n in (1, 2, 3)] + [on_ring(1), on_ring(-1), partner]
    for peer in peers:
        pl.semaphore_signal(barrier, inc=1, device_id=peer, device_id_type=pl.DeviceIdType.MESH)

    loads[0].wait()
    lane = lax.broadcasted_iota(jnp.int32, (1, 128), 1)
    row = jnp.zeros((1, 128), jnp.int32)
    for block in range(4):
        row = jnp.where(lane == block, idx_ref[block], row)
    idx_all[z, x] = row
    loads[1].wait()
    loads[2].wait()
    pl.semaphore_wait(barrier, len(peers))

    for way in (1, -1):
        tok_own(way, 0 if way > 0 else 1).start()
    for n in (1, 2, 3):
        index_x(n).start()
    for way in (1, -1):
        w_own(way, 0 if way > 0 else 1).start()

    to_scalars = pltpu.make_async_copy(idx_all, idx_s, local_sem.at[0])
    own_columns = pltpu.make_async_copy(up.at[:, :, up_columns(0)], spread.at[x], local_sem.at[1])

    def step_body(step, carry):
        @pl.when(step >= LAG_SUM)
        def _():
            done = step - LAG_SUM
            rows, columns = unit_of(done)
            for part in (0, 1):
                sum_copy(done, part).wait_recv()
            total = parts[done, y].astype(F32) + arrived[done, 0].astype(F32)
            total = (total + arrived[done, 1].astype(F32)).astype(BF)

            @pl.when(rows == 0)
            def _():
                for part in (0, 1):
                    final[z, (x + places_on(columns, part)) % 4, part] = total[part]

            @pl.when(rows > 0)
            def _():
                sums[done] = total
                for part in (0, 1):
                    final_copy(done, part).start()

        @pl.when((step >= LAG_RELAY) & (step < UNITS + LAG_RELAY))
        def _():
            done = step - LAG_RELAY
            for part in (0, 1):
                to = (y + (1 if part == 0 else 3)) % 4
                relay_copy(done, part).wait_recv()
                added = parts[done, to, part].astype(F32) + relay[done, part].astype(F32)
                parts[done, to, part] = added.astype(BF)

        @pl.when((step >= LAG_RELAY) & (step < UNITS + LAG_RELAY))
        def _():
            for part in (0, 1):
                sum_copy(step - LAG_RELAY, part).start()

        @pl.when(step == 1)
        def _():
            loads[3].wait()
            for block in range(4):
                chosen_down = down[idx_ref[block]]
                shr[block] = lax.dot_general(
                    chosen_down, toks[0, block], LAST, preferred_element_type=F32
                )
            for n in (1, 2, 3):
                shrink_copy(n).start()
            index_x_three.wait_recv()
            for n in (1, 2, 3):
                index_z(n).start()

        @pl.when(step == 1)
        def _():
            loads[4].wait()
            w_pair(1).wait_send()
            for way in (1, -1):
                part = 0 if way > 0 else 1
                up_near(way % 4).start()
                up_cross(part).start()
            tok_pair(1).wait_recv()
            for part in (0, 1):
                tok_forward(part).start()
                tok_partner(1, part).start()
            w_pair(1).wait_recv()

        @pl.when(step == 2)
        def _():
            up_three.wait_send()
            for way in (1, -1):
                part = 0 if way > 0 else 1
                w_own(way, 1 - part).start()
            tok_partner_arrival(1).wait_recv()

        @pl.when(step == 3)
        def _():
            tok_pair(3).wait_send()
            for way in (1, -1):
                tok_own(way, 1 if way > 0 else 0).start()

        @pl.when(step == 4)
        def _():
            tok_partner_arrival(3).wait_recv()

        @pl.when(step == 6)
        def _():
            w_pair(2).wait_recv()
            for part in (0, 1):
                w_forward(part).start()
            tok_pair(2).wait_recv()
            for part in (0, 1):
                tok_partner(2, part).start()

        @pl.when(step == 8)
        def _():
            tok_partner_arrival(2).wait_recv()

        @pl.when(step == 10)
        def _():
            w_pair(3).wait_recv()

        @pl.when(step < UNITS)
        def _():
            s, t = unit_of(step)
            result = lax.dot_general(
                wts[t].reshape(COLS, WIDTH), toks[s].reshape(4 * BLOCK, WIDTH), LAST,
                preferred_element_type=F32,
            ).astype(BF)
            for block in range(4):
                tile = result[:, block * BLOCK : (block + 1) * BLOCK]
                parts[step, block] = tile.reshape(2, HALF, BLOCK)

        @pl.when(step < UNITS)
        def _():
            for part in (0, 1):
                relay_copy(step, part).start()

        @pl.when(step == 3)
        def _():
            tok_pair(3).wait_recv()
            for part in (0, 1):
                tok_partner(3, part).start()
            up_transit.wait_recv()
            for part in (0, 1):
                up_relay(part).start()
            own_columns.start()

        @pl.when(step == PICK_STEP - 1)
        def _():
            index_z_three.wait_recv()
            to_scalars.start()

        @pl.when(step == PICK_STEP)
        def _():
            up_three.wait_recv()
            to_scalars.wait()
            own_columns.wait()
            for to_z in range(4):
                for to_x in range(4):
                    local = idx_s[to_z, to_x, 0, y] - 16 * z
                    owned = jnp.where((local >= 0) & (local < 16), 1.0, 0.0).astype(F32)
                    kept = jnp.clip(local, 0, 15)
                    factor = spread[kept // 4, kept % 4].astype(F32) * owned
                    picked[to_z, to_x] = factor.astype(BF)
            for part in (1, 0):
                up_pair(part).start()

        @pl.when(step == PAIR_STEP)
        def _():
            up_pair(1).wait_recv()
            for to_x in range(4):
                picked[3 - z, to_x] = picked[3 - z, to_x] + zpicks[1, to_x]
            up_far().start()

        @pl.when(step == FAR_STEP)
        def _():
            up_pair(0).wait_recv()
            up_far().wait_recv()
            for to_x in range(4):
                chosen[to_x] = (picked[z, to_x] + zpicks[0, to_x]) + zpicks[2, to_x]
            for n in (1, 2, 3):
                up_last(n).start()
            upfin[x] = chosen[x]

        return carry

    lax.fori_loop(0, UNITS + LAG_SUM, step_body, 0)

    def finish_sends():
        index_x_three.wait_send()
        index_z_three.wait_send()
        shrink_three.wait_send()
        up_transit.wait_send()
        remote(zpicks, zpicks, one.at[12], u2_r.at[0], partner).wait_send()
        up_last_three.wait_send()
        tok_pair(1).wait_send()
        tok_pair(2).wait_send()
        w_pair(2).wait_send()
        w_pair(3).wait_send()
        passed = toks.at[pl.ds(1, 3), pl.ds(0, 2)]
        remote(passed, passed, one.at[0], tokp_r.at[0], partner).wait_send()
        remote(relay, relay, one.at[1], r1_r.at[0, 0], partner).wait_send()
        remote(arrived, arrived, one.at[2], r2_r.at[0, 0], partner).wait_send()

    shrink_three.wait_recv()
    low = (shr[y] + shr_in[0] + (shr_in[1] + shr_in[2])).astype(BF)
    same = lax.broadcasted_iota(jnp.int32, (BLOCK, BLOCK), 0) == lax.broadcasted_iota(
        jnp.int32, (BLOCK, BLOCK), 1
    )
    eye = jnp.where(same, 1.0, 0.0).astype(BF)
    turned = lax.dot_general(eye, low, LAST, preferred_element_type=F32)
    doubled = (2.0 * turned).astype(BF)
    loads[5].wait()
    live = lax.broadcasted_iota(jnp.int32, (BLOCK, 1), 0) < live_ref[y]
    up_last_three.wait_recv()

    for n in (0, 1, 3, 2):
        place = (z + n) % 4
        if n:
            final_arrival(place).wait_recv()
        base = lax.dot_general(
            eye, final[place].reshape(SLICE, BLOCK), LAST, preferred_element_type=F32
        )
        extra = jnp.dot(doubled, upfin[place], preferred_element_type=F32)
        columns = pl.ds(pl.multiple_of(place * SLICE, SLICE), SLICE)
        out_ref[:, columns] = jnp.where(live, base + extra, 0.0).astype(BF)
        if n == 0:
            finish_sends()
    gone = sums.at[pl.ds(*AWAY)]
    remote(gone, gone, one.at[3], fin_r.at[z], partner).wait_send()


def body(tokens, base_up_weight, adapter_down_weight, adapter_up_weight, block_adapter_index, request_rows):
    dma = pltpu.SemaphoreType.DMA
    half_tile = (2, HALF, BLOCK)
    any_space = pl.BlockSpec(memory_space=pl.ANY)
    return pl.pallas_call(
        kernel,
        out_shape=pltpu.VMEM((BLOCK, 4 * SLICE), BF),
        in_specs=[any_space] * 6,
        out_specs=pl.BlockSpec(memory_space=pltpu.VMEM),
        scratch_shapes=[
            pltpu.VMEM((4, 4, BLOCK, WIDTH), BF),
            pltpu.VMEM((4, 2, HALF, WIDTH), BF),
            pltpu.VMEM((CATALOG, RANK, WIDTH), BF),
            pltpu.VMEM((4, RANK, 4 * SLICE), BF),
            pltpu.VMEM((UNITS, 4, *half_tile), BF),
            pltpu.VMEM((UNITS, *half_tile), BF),
            pltpu.VMEM((UNITS, 2, *half_tile), BF),
            pltpu.VMEM((UNITS, *half_tile), BF),
            pltpu.VMEM((4, 4, *half_tile), BF),
            pltpu.VMEM((4, RANK, SLICE), BF),
            pltpu.SMEM((4,), jnp.int32),
            pltpu.SMEM((4,), jnp.int32),
            pltpu.VMEM((4, 4, 1, 128), jnp.int32),
            pltpu.SMEM((4, 4, 1, 128), jnp.int32),
            pltpu.VMEM((4, 4, RANK, SLICE), BF),
            pltpu.VMEM((2, 2, RANK, SLICE), BF),
            pltpu.VMEM((4, 4, RANK, SLICE), BF),
            pltpu.VMEM((3, 4, RANK, SLICE), BF),
            pltpu.VMEM((4, RANK, SLICE), BF),
            pltpu.VMEM((4, RANK, BLOCK), F32),
            pltpu.VMEM((3, RANK, BLOCK), F32),
            dma((6,)), dma((17,)),
            dma((3,)), dma((3,)), dma((3,)), dma((3,)), dma((3,)),
            dma((4, 2)), dma((4, 2)), dma((4,)), dma((3,)),
        ],
        compiler_params=pltpu.CompilerParams(
            collective_id=0, has_side_effects=True, vmem_limit_bytes=60000000
        ),
    )(
        block_adapter_index,
        request_rows,
        tokens.reshape(4, BLOCK, WIDTH),
        base_up_weight.T.reshape(2, HALF, WIDTH),
        adapter_down_weight,
        adapter_up_weight,
    )


def solution(mesh):
    in_specs = (
        P("gx", "gy"),
        P("gy", ("gz", "gx")),
        P(None, None, "gy"),
        P("gx", None, "gz"),
        P("gx"),
        P("gx"),
    )
    out_specs = P(("gx", "gy"), "gz")
    return jax.shard_map(body, mesh=mesh, in_specs=in_specs, out_specs=out_specs, check_vma=False)
```

```python
import functools

import jax
import jax.numpy as jnp
from jax import lax
from jax.experimental import pallas as pl
from jax.experimental.pallas import tpu as pltpu
from jax.sharding import PartitionSpec as P

BLOCK = 128
RANK = 16
CATALOG = 64
WIDTH = 1152
COLS = 288
HALF = COLS // 2
SLICE = 4 * COLS
UNITS = 16
LAG_RELAY = 2
LAG_SUM = 4
PICK_STEP = 5
PAIR_STEP = 7
FAR_STEP = 16
AWAY = (2, 12)
BF = jnp.bfloat16
F32 = jnp.float32
LAST = (((1,), (1,)), ((), ()))


ORDER = (
    (0, 0), (0, 1), (1, 0), (1, 1), (3, 0), (3, 1), (1, 2), (3, 2),
    (2, 0), (2, 1), (3, 3), (1, 3), (2, 2), (2, 3), (0, 2), (0, 3),
)


def staircase(step, column):
    rises = [(at, ORDER[at][column] - ORDER[at - 1][column]) for at in range(1, UNITS)]
    return sum(rise * ((step + 16 - at) // 16) for at, rise in rises if rise)


def unit_of(step):
    return staircase(step, 0), staircase(step, 1)


def places_on(kind, part):
    three = kind // 3
    two = kind // 2 - three
    one = kind - 2 * (kind // 2) - three
    return one * (3 - 2 * part) + two * (1 + 2 * part) + 2 * three


def kernel(
    idx_hbm, live_hbm, tok_hbm, wt_hbm, down_hbm, up_hbm, out_ref,
    toks, wts, down, up, parts, relay, arrived, sums, final, upfin,
    idx_ref, live_ref, idx_all, idx_s, spread, transit, picked, zpicks, chosen, shr, shr_in,
    local_sem, one, tok_s, tok_r, tokp_r, w_s, w_r, r1_r, r2_r, fin_r, u2_r,
):
    gx = lax.axis_index("gx")
    y = lax.axis_index("gy")
    gz = lax.axis_index("gz")
    z, x = gx // 4, gx % 4
    zh, core = gz // 2, gz % 2
    ring = zh * 4 + z

    def along_x(step):
        return (z * 4 + (x + step) % 4, y, gz)

    def along_y(step):
        return (gx, (y + step) % 4, gz)

    def along_z(step):
        return (((z + step) % 4) * 4 + x, y, gz)

    def on_ring(step):
        place = (ring + step) % 8
        return ((place % 4) * 4 + x, y, (place // 4) * 2 + core)

    partner = (gx, y, zh * 2 + 1 - core)

    def remote(src, dst, send, recv, to):
        return pltpu.make_async_remote_copy(
            src_ref=src, dst_ref=dst, send_sem=send, recv_sem=recv,
            device_id=to, device_id_type=pl.DeviceIdType.MESH,
        )

    def kind_of(way, part):
        return 1 if (way > 0) == (part == 0) else 2

    def tok_own(way, part):
        kind, block = kind_of(way, part), 2 * core + part
        return remote(
            toks.at[0, block], toks.at[kind, block],
            tok_s.at[kind - 1], tok_r.at[kind - 1], on_ring(way),
        )

    def tok_forward(part):
        block = 2 * core + part
        return remote(
            toks.at[1, block], toks.at[3, block],
            tok_s.at[2], tok_r.at[2], on_ring(1 if part == 0 else -1),
        )

    def tok_partner(kind, part):
        block = 2 * core + part
        return remote(
            toks.at[kind, block], toks.at[kind, block], one.at[0], tokp_r.at[kind - 1], partner
        )

    def tok_pair(kind):
        blocks = pl.ds(2 * core, 2)
        return remote(
            toks.at[kind, blocks], toks.at[kind, blocks], tok_s.at[kind - 1], tok_r.at[kind - 1], partner
        )

    def tok_partner_arrival(kind):
        blocks = pl.ds(2 * (1 - core), 2)
        return remote(
            toks.at[kind, blocks], toks.at[kind, blocks], one.at[0], tokp_r.at[kind - 1], partner
        )

    def w_own(way, part):
        kind = kind_of(way, part)
        return remote(
            wts.at[0, part], wts.at[kind, part],
            w_s.at[kind - 1], w_r.at[kind - 1], along_x(way % 4),
        )

    def w_forward(part):
        return remote(
            wts.at[1, part], wts.at[3, part],
            w_s.at[2], w_r.at[2], along_x(1 if part == 0 else 3),
        )

    def w_pair(kind):
        return remote(wts.at[kind], wts.at[kind], w_s.at[kind - 1], w_r.at[kind - 1], along_x(1))

    def relay_copy(step, part):
        return remote(
            parts.at[step, (y + 2) % 4, part], relay.at[step, part],
            one.at[1], r1_r.at[step % 4, part], along_y(1 if part == 0 else 3),
        )

    def sum_copy(step, part):
        way = 1 if part == 0 else 3
        return remote(
            parts.at[step, (y + way) % 4], arrived.at[step, part],
            one.at[2], r2_r.at[step % 4, part], along_y(way),
        )

    def final_copy(step, part):
        rows, columns = unit_of(step)
        chunk = (x + places_on(columns, part)) % 4
        return remote(
            sums.at[step, part], final.at[z, chunk, part],
            one.at[3], fin_r.at[z], along_z(places_on(rows, y % 2)),
        )

    def final_arrival(place):
        return remote(final.at[place], final.at[place], one.at[3], fin_r.at[place], along_z(1))

    def index_x(step):
        return remote(idx_all.at[z, x], idx_all.at[z, x], one.at[4], one.at[5], along_x(step))

    def index_z(step):
        return remote(idx_all.at[z], idx_all.at[z], one.at[6], one.at[7], along_z(step))

    index_x_three = remote(
        idx_all.at[0, pl.ds(0, 3)], idx_all.at[0, pl.ds(0, 3)], one.at[4], one.at[5], along_x(1)
    )
    index_z_three = remote(
        idx_all.at[pl.ds(0, 3)], idx_all.at[pl.ds(0, 3)], one.at[6], one.at[7], along_z(1)
    )

    def up_columns(step):
        return pl.ds(pl.multiple_of((x + step) % 4 * SLICE, SLICE), SLICE)

    def up_near(step):
        return remote(up.at[:, :, up_columns(step)], spread.at[x], one.at[8], one.at[9], along_x(step))

    def up_cross(part):
        return remote(
            up.at[pl.ds(2 * part, 2), :, up_columns(2)], transit.at[part],
            one.at[8], one.at[10], along_x(1 if part == 0 else 3),
        )

    def up_relay(part):
        step = 1 if part == 0 else 3
        place = (x + 4 - step) % 4
        return remote(
            transit.at[part], spread.at[place, pl.ds(2 * part, 2)],
            one.at[11], one.at[9], along_x(step),
        )

    up_three = remote(spread.at[pl.ds(0, 3)], spread.at[pl.ds(0, 3)], one.at[8], one.at[9], along_x(1))
    up_transit = remote(transit, transit, one.at[11], one.at[10], along_x(1))

    mate = 1 - 2 * (z % 2)
    far = 3 - 2 * z

    def up_pair(part):
        chunk = z + mate if part == 0 else 3 - (z + mate)
        return remote(
            picked.at[chunk], zpicks.at[part], one.at[12], u2_r.at[part], along_z(mate + 4)
        )

    def up_far():
        return remote(picked.at[3 - z], zpicks.at[2], one.at[12], u2_r.at[2], along_z(far + 4))

    def up_last(step):
        return remote(
            chosen.at[(x + step) % 4], upfin.at[x], one.at[13], one.at[14], along_x(step)
        )

    def shrink_copy(step):
        return remote(
            shr.at[(y + step) % 4], shr_in.at[step - 1], one.at[15], one.at[16], along_y(step)
        )

    up_last_three = remote(
        chosen.at[pl.ds(0, 3)], upfin.at[pl.ds(0, 3)], one.at[13], one.at[14], along_x(1)
    )
    shrink_three = remote(shr_in, shr_in, one.at[15], one.at[16], along_y(1))

    loads = [
        pltpu.make_async_copy(idx_hbm, idx_ref, local_sem.at[4]),
        pltpu.make_async_copy(tok_hbm, toks.at[0], local_sem.at[0]),
        pltpu.make_async_copy(wt_hbm, wts.at[0], local_sem.at[1]),
        pltpu.make_async_copy(down_hbm, down, local_sem.at[2]),
        pltpu.make_async_copy(up_hbm, up, local_sem.at[3]),
        pltpu.make_async_copy(live_hbm, live_ref, local_sem.at[5]),
    ]
    for load in loads:
        load.start()
    barrier = pltpu.get_barrier_semaphore()
    peers = [along_x(n) for n in (1, 2, 3)] + [along_y(n) for n in (1, 2, 3)]
    peers += [along_z(n) for n in (1, 2, 3)] + [on_ring(1), on_ring(-1), partner]
    for peer in peers:
        pl.semaphore_signal(barrier, inc=1, device_id=peer, device_id_type=pl.DeviceIdType.MESH)

    loads[0].wait()
    lane = lax.broadcasted_iota(jnp.int32, (1, 128), 1)
    row = jnp.zeros((1, 128), jnp.int32)
    for block in range(4):
        row = jnp.where(lane == block, idx_ref[block], row)
    idx_all[z, x] = row
    loads[1].wait()
    loads[2].wait()
    pl.semaphore_wait(barrier, len(peers))

    for way in (1, -1):
        tok_own(way, 0 if way > 0 else 1).start()
    for n in (1, 2, 3):
        index_x(n).start()
    for way in (1, -1):
        w_own(way, 0 if way > 0 else 1).start()

    to_scalars = pltpu.make_async_copy(idx_all, idx_s, local_sem.at[0])
    own_columns = pltpu.make_async_copy(up.at[:, :, up_columns(0)], spread.at[x], local_sem.at[1])

    def step_body(step, carry):
        @pl.when(step >= LAG_SUM)
        def _():
            done = step - LAG_SUM
            rows, columns = unit_of(done)
            for part in (0, 1):
                sum_copy(done, part).wait_recv()
            total = parts[done, y].astype(F32) + arrived[done, 0].astype(F32)
            total = (total + arrived[done, 1].astype(F32)).astype(BF)

            @pl.when(rows == 0)
            def _():
                for part in (0, 1):
                    final[z, (x + places_on(columns, part)) % 4, part] = total[part]

            @pl.when(rows > 0)
            def _():
                sums[done] = total
                for part in (0, 1):
                    final_copy(done, part).start()

        @pl.when((step >= LAG_RELAY) & (step < UNITS + LAG_RELAY))
        def _():
            done = step - LAG_RELAY
            for part in (0, 1):
                to = (y + (1 if part == 0 else 3)) % 4
                relay_copy(done, part).wait_recv()
                added = parts[done, to, part].astype(F32) + relay[done, part].astype(F32)
                parts[done, to, part] = added.astype(BF)

        @pl.when((step >= LAG_RELAY) & (step < UNITS + LAG_RELAY))
        def _():
            for part in (0, 1):
                sum_copy(step - LAG_RELAY, part).start()

        @pl.when(step == 1)
        def _():
            loads[3].wait()
            for block in range(4):
                chosen_down = down[idx_ref[block]]
                shr[block] = lax.dot_general(
                    chosen_down, toks[0, block], LAST, preferred_element_type=F32
                )
            for n in (1, 2, 3):
                shrink_copy(n).start()
            index_x_three.wait_recv()
            for n in (1, 2, 3):
                index_z(n).start()

        @pl.when(step == 1)
        def _():
            loads[4].wait()
            w_pair(1).wait_send()
            for way in (1, -1):
                part = 0 if way > 0 else 1
                up_near(way % 4).start()
                up_cross(part).start()
            tok_pair(1).wait_recv()
            for part in (0, 1):
                tok_forward(part).start()
                tok_partner(1, part).start()
            w_pair(1).wait_recv()

        @pl.when(step == 2)
        def _():
            up_three.wait_send()
            for way in (1, -1):
                part = 0 if way > 0 else 1
                w_own(way, 1 - part).start()
            tok_partner_arrival(1).wait_recv()

        @pl.when(step == 3)
        def _():
            tok_pair(3).wait_send()
            for way in (1, -1):
                tok_own(way, 1 if way > 0 else 0).start()

        @pl.when(step == 4)
        def _():
            tok_partner_arrival(3).wait_recv()

        @pl.when(step == 6)
        def _():
            w_pair(2).wait_recv()
            for part in (0, 1):
                w_forward(part).start()
            tok_pair(2).wait_recv()
            for part in (0, 1):
                tok_partner(2, part).start()

        @pl.when(step == 8)
        def _():
            tok_partner_arrival(2).wait_recv()

        @pl.when(step == 10)
        def _():
            w_pair(3).wait_recv()

        @pl.when(step < UNITS)
        def _():
            s, t = unit_of(step)
            result = lax.dot_general(
                wts[t].reshape(COLS, WIDTH), toks[s].reshape(4 * BLOCK, WIDTH), LAST,
                preferred_element_type=F32,
            ).astype(BF)
            for block in range(4):
                tile = result[:, block * BLOCK : (block + 1) * BLOCK]
                parts[step, block] = tile.reshape(2, HALF, BLOCK)

        @pl.when(step < UNITS)
        def _():
            for part in (0, 1):
                relay_copy(step, part).start()

        @pl.when(step == 3)
        def _():
            tok_pair(3).wait_recv()
            for part in (0, 1):
                tok_partner(3, part).start()
            up_transit.wait_recv()
            for part in (0, 1):
                up_relay(part).start()
            own_columns.start()

        @pl.when(step == PICK_STEP - 1)
        def _():
            index_z_three.wait_recv()
            to_scalars.start()

        @pl.when(step == PICK_STEP)
        def _():
            up_three.wait_recv()
            to_scalars.wait()
            own_columns.wait()
            for to_z in range(4):
                for to_x in range(4):
                    local = idx_s[to_z, to_x, 0, y] - 16 * z
                    owned = jnp.where((local >= 0) & (local < 16), 1.0, 0.0).astype(F32)
                    kept = jnp.clip(local, 0, 15)
                    factor = spread[kept // 4, kept % 4].astype(F32) * owned
                    picked[to_z, to_x] = factor.astype(BF)
            for part in (1, 0):
                up_pair(part).start()

        @pl.when(step == PAIR_STEP)
        def _():
            up_pair(1).wait_recv()
            for to_x in range(4):
                picked[3 - z, to_x] = picked[3 - z, to_x] + zpicks[1, to_x]
            up_far().start()

        @pl.when(step == FAR_STEP)
        def _():
            up_pair(0).wait_recv()
            up_far().wait_recv()
            for to_x in range(4):
                chosen[to_x] = (picked[z, to_x] + zpicks[0, to_x]) + zpicks[2, to_x]
            for n in (1, 2, 3):
                up_last(n).start()
            upfin[x] = chosen[x]

        return carry

    lax.fori_loop(0, UNITS + LAG_SUM, step_body, 0)

    def finish_sends():
        index_x_three.wait_send()
        index_z_three.wait_send()
        shrink_three.wait_send()
        up_transit.wait_send()
        remote(zpicks, zpicks, one.at[12], u2_r.at[0], partner).wait_send()
        up_last_three.wait_send()
        tok_pair(1).wait_send()
        tok_pair(2).wait_send()
        w_pair(2).wait_send()
        w_pair(3).wait_send()
        passed = toks.at[pl.ds(1, 3), pl.ds(0, 2)]
        remote(passed, passed, one.at[0], tokp_r.at[0], partner).wait_send()
        remote(relay, relay, one.at[1], r1_r.at[0, 0], partner).wait_send()
        remote(arrived, arrived, one.at[2], r2_r.at[0, 0], partner).wait_send()

    shrink_three.wait_recv()
    low = (shr[y] + shr_in[0] + (shr_in[1] + shr_in[2])).astype(BF)
    same = lax.broadcasted_iota(jnp.int32, (BLOCK, BLOCK), 0) == lax.broadcasted_iota(
        jnp.int32, (BLOCK, BLOCK), 1
    )
    eye = jnp.where(same, 1.0, 0.0).astype(BF)
    turned = lax.dot_general(eye, low, LAST, preferred_element_type=F32)
    doubled = (2.0 * turned).astype(BF)
    loads[5].wait()
    live = lax.broadcasted_iota(jnp.int32, (BLOCK, 1), 0) < live_ref[y]
    up_last_three.wait_recv()

    for n in (0, 2, 1, 3):
        place = (z + n) % 4
        if n:
            final_arrival(place).wait_recv()
        base = lax.dot_general(
            eye, final[place].reshape(SLICE, BLOCK), LAST, preferred_element_type=F32
        )
        extra = jnp.dot(doubled, upfin[place], preferred_element_type=F32)
        columns = pl.ds(pl.multiple_of(place * SLICE, SLICE), SLICE)
        out_ref[:, columns] = jnp.where(live, base + extra, 0.0).astype(BF)
        if n == 0:
            finish_sends()
    gone = sums.at[pl.ds(*AWAY)]
    remote(gone, gone, one.at[3], fin_r.at[z], partner).wait_send()


def body(tokens, base_up_weight, adapter_down_weight, adapter_up_weight, block_adapter_index, request_rows):
    dma = pltpu.SemaphoreType.DMA
    half_tile = (2, HALF, BLOCK)
    any_space = pl.BlockSpec(memory_space=pl.ANY)
    return pl.pallas_call(
        kernel,
        out_shape=pltpu.VMEM((BLOCK, 4 * SLICE), BF),
        in_specs=[any_space] * 6,
        out_specs=pl.BlockSpec(memory_space=pltpu.VMEM),
        scratch_shapes=[
            pltpu.VMEM((4, 4, BLOCK, WIDTH), BF),
            pltpu.VMEM((4, 2, HALF, WIDTH), BF),
            pltpu.VMEM((CATALOG, RANK, WIDTH), BF),
            pltpu.VMEM((4, RANK, 4 * SLICE), BF),
            pltpu.VMEM((UNITS, 4, *half_tile), BF),
            pltpu.VMEM((UNITS, *half_tile), BF),
            pltpu.VMEM((UNITS, 2, *half_tile), BF),
            pltpu.VMEM((UNITS, *half_tile), BF),
            pltpu.VMEM((4, 4, *half_tile), BF),
            pltpu.VMEM((4, RANK, SLICE), BF),
            pltpu.SMEM((4,), jnp.int32),
            pltpu.SMEM((4,), jnp.int32),
            pltpu.VMEM((4, 4, 1, 128), jnp.int32),
            pltpu.SMEM((4, 4, 1, 128), jnp.int32),
            pltpu.VMEM((4, 4, RANK, SLICE), BF),
            pltpu.VMEM((2, 2, RANK, SLICE), BF),
            pltpu.VMEM((4, 4, RANK, SLICE), BF),
            pltpu.VMEM((3, 4, RANK, SLICE), BF),
            pltpu.VMEM((4, RANK, SLICE), BF),
            pltpu.VMEM((4, RANK, BLOCK), F32),
            pltpu.VMEM((3, RANK, BLOCK), F32),
            dma((6,)), dma((17,)),
            dma((3,)), dma((3,)), dma((3,)), dma((3,)), dma((3,)),
            dma((4, 2)), dma((4, 2)), dma((4,)), dma((3,)),
        ],
        compiler_params=pltpu.CompilerParams(
            collective_id=0, has_side_effects=True, vmem_limit_bytes=60000000
        ),
    )(
        block_adapter_index,
        request_rows,
        tokens.reshape(4, BLOCK, WIDTH),
        base_up_weight.T.reshape(2, HALF, WIDTH),
        adapter_down_weight,
        adapter_up_weight,
    )


def solution(mesh):
    in_specs = (
        P("gx", "gy"),
        P("gy", ("gz", "gx")),
        P(None, None, "gy"),
        P("gx", None, "gz"),
        P("gx"),
        P("gx"),
    )
    out_specs = P(("gx", "gy"), "gz")
    return jax.shard_map(body, mesh=mesh, in_specs=in_specs, out_specs=out_specs, check_vma=False)
```

```python
import functools

import jax
import jax.numpy as jnp
from jax import lax
from jax.experimental import pallas as pl
from jax.experimental.pallas import tpu as pltpu
from jax.sharding import PartitionSpec as P

BLOCK = 128
RANK = 16
CATALOG = 64
WIDTH = 1152
COLS = 288
HALF = COLS // 2
SLICE = 4 * COLS
UNITS = 16
LAG_RELAY = 2
LAG_SUM = 4
PICK_STEP = 5
PAIR_STEP = 7
FAR_STEP = 16
AWAY = (2, 12)
BF = jnp.bfloat16
F32 = jnp.float32
LAST = (((1,), (1,)), ((), ()))


ORDER = (
    (0, 0), (0, 1), (1, 0), (1, 1), (3, 0), (3, 1), (1, 2), (3, 2),
    (2, 0), (2, 1), (3, 3), (1, 3), (2, 2), (2, 3), (0, 2), (0, 3),
)


def staircase(step, column):
    rises = [(at, ORDER[at][column] - ORDER[at - 1][column]) for at in range(1, UNITS)]
    return sum(rise * ((step + 16 - at) // 16) for at, rise in rises if rise)


def unit_of(step):
    return staircase(step, 0), staircase(step, 1)


def places_on(kind, part):
    three = kind // 3
    two = kind // 2 - three
    one = kind - 2 * (kind // 2) - three
    return one * (3 - 2 * part) + two * (1 + 2 * part) + 2 * three


def kernel(
    idx_hbm, live_hbm, tok_hbm, wt_hbm, down_hbm, up_hbm, out_ref,
    toks, wts, down, up, parts, relay, arrived, sums, final, upfin,
    idx_ref, live_ref, idx_all, idx_s, spread, transit, picked, zpicks, chosen, shr, shr_in,
    local_sem, one, tok_s, tok_r, tokp_r, w_s, w_r, r1_r, r2_r, fin_r, u2_r,
):
    gx = lax.axis_index("gx")
    y = lax.axis_index("gy")
    gz = lax.axis_index("gz")
    z, x = gx // 4, gx % 4
    zh, core = gz // 2, gz % 2
    ring = zh * 4 + z

    def along_x(step):
        return (z * 4 + (x + step) % 4, y, gz)

    def along_y(step):
        return (gx, (y + step) % 4, gz)

    def along_z(step):
        return (((z + step) % 4) * 4 + x, y, gz)

    def on_ring(step):
        place = (ring + step) % 8
        return ((place % 4) * 4 + x, y, (place // 4) * 2 + core)

    partner = (gx, y, zh * 2 + 1 - core)

    def remote(src, dst, send, recv, to):
        return pltpu.make_async_remote_copy(
            src_ref=src, dst_ref=dst, send_sem=send, recv_sem=recv,
            device_id=to, device_id_type=pl.DeviceIdType.MESH,
        )

    def kind_of(way, part):
        return 1 if (way > 0) == (part == 0) else 2

    def tok_own(way, part):
        kind, block = kind_of(way, part), 2 * core + part
        return remote(
            toks.at[0, block], toks.at[kind, block],
            tok_s.at[kind - 1], tok_r.at[kind - 1], on_ring(way),
        )

    def tok_forward(part):
        block = 2 * core + part
        return remote(
            toks.at[1, block], toks.at[3, block],
            tok_s.at[2], tok_r.at[2], on_ring(1 if part == 0 else -1),
        )

    def tok_partner(kind, part):
        block = 2 * core + part
        return remote(
            toks.at[kind, block], toks.at[kind, block], one.at[0], tokp_r.at[kind - 1], partner
        )

    def tok_pair(kind):
        blocks = pl.ds(2 * core, 2)
        return remote(
            toks.at[kind, blocks], toks.at[kind, blocks], tok_s.at[kind - 1], tok_r.at[kind - 1], partner
        )

    def tok_second(block):
        return remote(
            toks.at[0, block], toks.at[2, block],
            tok_s.at[1], tok_r.at[1], on_ring(1 if block % 2 else -1),
        )

    tok_seconds = remote(toks.at[2], toks.at[2], tok_s.at[1], tok_r.at[1], partner)
    tok_seconds_pass = remote(toks.at[2], toks.at[2], one.at[17], tokp_r.at[1], partner)

    def tok_partner_arrival(kind):
        blocks = pl.ds(2 * (1 - core), 2)
        return remote(
            toks.at[kind, blocks], toks.at[kind, blocks], one.at[0], tokp_r.at[kind - 1], partner
        )

    def w_own(way, part):
        kind = kind_of(way, part)
        return remote(
            wts.at[0, part], wts.at[kind, part],
            w_s.at[kind - 1], w_r.at[kind - 1], along_x(way % 4),
        )

    def w_forward(part):
        return remote(
            wts.at[1, part], wts.at[3, part],
            w_s.at[2], w_r.at[2], along_x(1 if part == 0 else 3),
        )

    def w_pair(kind):
        return remote(wts.at[kind], wts.at[kind], w_s.at[kind - 1], w_r.at[kind - 1], along_x(1))

    def relay_copy(step, part):
        return remote(
            parts.at[step, (y + 2) % 4, part], relay.at[step, part],
            one.at[1], r1_r.at[step % 4, part], along_y(1 if part == 0 else 3),
        )

    def sum_copy(step, part):
        way = 1 if part == 0 else 3
        return remote(
            parts.at[step, (y + way) % 4], arrived.at[step, part],
            one.at[2], r2_r.at[step % 4, part], along_y(way),
        )

    def final_copy(step, part):
        rows, columns = unit_of(step)
        chunk = (x + places_on(columns, part)) % 4
        return remote(
            sums.at[step, part], final.at[z, chunk, part],
            one.at[3], fin_r.at[z], along_z(places_on(rows, y % 2)),
        )

    def final_arrival(place):
        return remote(final.at[place], final.at[place], one.at[3], fin_r.at[place], along_z(1))

    def index_x(step):
        return remote(idx_all.at[z, x], idx_all.at[z, x], one.at[4], one.at[5], along_x(step))

    def index_z(step):
        return remote(idx_all.at[z], idx_all.at[z], one.at[6], one.at[7], along_z(step))

    index_x_three = remote(
        idx_all.at[0, pl.ds(0, 3)], idx_all.at[0, pl.ds(0, 3)], one.at[4], one.at[5], along_x(1)
    )
    index_z_three = remote(
        idx_all.at[pl.ds(0, 3)], idx_all.at[pl.ds(0, 3)], one.at[6], one.at[7], along_z(1)
    )

    def up_columns(step):
        return pl.ds(pl.multiple_of((x + step) % 4 * SLICE, SLICE), SLICE)

    def up_near(step):
        return remote(up.at[:, :, up_columns(step)], spread.at[x], one.at[8], one.at[9], along_x(step))

    def up_cross(part):
        return remote(
            up.at[pl.ds(2 * part, 2), :, up_columns(2)], transit.at[part],
            one.at[8], one.at[10], along_x(1 if part == 0 else 3),
        )

    def up_relay(part):
        step = 1 if part == 0 else 3
        place = (x + 4 - step) % 4
        return remote(
            transit.at[part], spread.at[place, pl.ds(2 * part, 2)],
            one.at[11], one.at[9], along_x(step),
        )

    up_three = remote(spread.at[pl.ds(0, 3)], spread.at[pl.ds(0, 3)], one.at[8], one.at[9], along_x(1))
    up_transit = remote(transit, transit, one.at[11], one.at[10], along_x(1))

    mate = 1 - 2 * (z % 2)
    far = 3 - 2 * z

    def up_pair(part):
        chunk = z + mate if part == 0 else 3 - (z + mate)
        return remote(
            picked.at[chunk], zpicks.at[part], one.at[12], u2_r.at[part], along_z(mate + 4)
        )

    def up_far():
        return remote(picked.at[3 - z], zpicks.at[2], one.at[12], u2_r.at[2], along_z(far + 4))

    def up_last(step):
        return remote(
            chosen.at[(x + step) % 4], upfin.at[x], one.at[13], one.at[14], along_x(step)
        )

    def shrink_copy(step):
        return remote(
            shr.at[(y + step) % 4], shr_in.at[step - 1], one.at[15], one.at[16], along_y(step)
        )

    up_last_three = remote(
        chosen.at[pl.ds(0, 3)], upfin.at[pl.ds(0, 3)], one.at[13], one.at[14], along_x(1)
    )
    shrink_three = remote(shr_in, shr_in, one.at[15], one.at[16], along_y(1))

    loads = [
        pltpu.make_async_copy(idx_hbm, idx_ref, local_sem.at[4]),
        pltpu.make_async_copy(tok_hbm, toks.at[0], local_sem.at[0]),
        pltpu.make_async_copy(wt_hbm, wts.at[0], local_sem.at[1]),
        pltpu.make_async_copy(down_hbm, down, local_sem.at[2]),
        pltpu.make_async_copy(up_hbm, up, local_sem.at[3]),
        pltpu.make_async_copy(live_hbm, live_ref, local_sem.at[5]),
    ]
    for load in loads:
        load.start()
    barrier = pltpu.get_barrier_semaphore()
    peers = [along_x(n) for n in (1, 2, 3)] + [along_y(n) for n in (1, 2, 3)]
    peers += [along_z(n) for n in (1, 2, 3)] + [on_ring(1), on_ring(-1), partner]
    for peer in peers:
        pl.semaphore_signal(barrier, inc=1, device_id=peer, device_id_type=pl.DeviceIdType.MESH)

    loads[0].wait()
    lane = lax.broadcasted_iota(jnp.int32, (1, 128), 1)
    row = jnp.zeros((1, 128), jnp.int32)
    for block in range(4):
        row = jnp.where(lane == block, idx_ref[block], row)
    idx_all[z, x] = row
    loads[1].wait()
    loads[2].wait()
    pl.semaphore_wait(barrier, len(peers))

    for way in (1, -1):
        tok_own(way, 0 if way > 0 else 1).start()
    for n in (1, 2, 3):
        index_x(n).start()
    for way in (1, -1):
        w_own(way, 0 if way > 0 else 1).start()

    to_scalars = pltpu.make_async_copy(idx_all, idx_s, local_sem.at[0])
    own_columns = pltpu.make_async_copy(up.at[:, :, up_columns(0)], spread.at[x], local_sem.at[1])

    def step_body(step, carry):
        @pl.when(step >= LAG_SUM)
        def _():
            done = step - LAG_SUM
            rows, columns = unit_of(done)
            for part in (0, 1):
                sum_copy(done, part).wait_recv()
            total = parts[done, y].astype(F32) + arrived[done, 0].astype(F32)
            total = (total + arrived[done, 1].astype(F32)).astype(BF)

            @pl.when(rows == 0)
            def _():
                for part in (0, 1):
                    final[z, (x + places_on(columns, part)) % 4, part] = total[part]

            @pl.when(rows > 0)
            def _():
                sums[done] = total
                for part in (0, 1):
                    final_copy(done, part).start()

        @pl.when((step >= LAG_RELAY) & (step < UNITS + LAG_RELAY))
        def _():
            done = step - LAG_RELAY
            for part in (0, 1):
                to = (y + (1 if part == 0 else 3)) % 4
                relay_copy(done, part).wait_recv()
                added = parts[done, to, part].astype(F32) + relay[done, part].astype(F32)
                parts[done, to, part] = added.astype(BF)

        @pl.when((step >= LAG_RELAY) & (step < UNITS + LAG_RELAY))
        def _():
            for part in (0, 1):
                sum_copy(step - LAG_RELAY, part).start()

        @pl.when(step == 1)
        def _():
            loads[3].wait()
            for block in range(4):
                chosen_down = down[idx_ref[block]]
                shr[block] = lax.dot_general(
                    chosen_down, toks[0, block], LAST, preferred_element_type=F32
                )
            for n in (1, 2, 3):
                shrink_copy(n).start()
            index_x_three.wait_recv()
            for n in (1, 2, 3):
                index_z(n).start()

        @pl.when(step == 1)
        def _():
            loads[4].wait()
            w_pair(1).wait_send()
            for way in (1, -1):
                part = 0 if way > 0 else 1
                up_near(way % 4).start()
                up_cross(part).start()
            tok_pair(1).wait_recv()
            for part in (0, 1):
                tok_forward(part).start()
                tok_partner(1, part).start()
            w_pair(1).wait_recv()

        @pl.when(step == 2)
        def _():
            up_three.wait_send()
            for way in (1, -1):
                part = 0 if way > 0 else 1
                w_own(way, 1 - part).start()
            tok_partner_arrival(1).wait_recv()

        @pl.when(step == 3)
        def _():
            tok_pair(3).wait_send()

            @pl.when(core == 1)
            def _():
                for block in range(4):
                    tok_second(block).start()


        @pl.when(step == 4)
        def _():
            tok_partner_arrival(3).wait_recv()

        @pl.when(step == 6)
        def _():
            w_pair(2).wait_recv()
            for part in (0, 1):
                w_forward(part).start()

            @pl.when(core == 1)
            def _():
                tok_seconds.wait_recv()
                tok_seconds_pass.start()


        @pl.when(step == 8)
        def _():

            @pl.when(core == 0)
            def _():
                tok_seconds_pass.wait_recv()


        @pl.when(step == 10)
        def _():
            w_pair(3).wait_recv()

        @pl.when(step < UNITS)
        def _():
            s, t = unit_of(step)
            result = lax.dot_general(
                wts[t].reshape(COLS, WIDTH), toks[s].reshape(4 * BLOCK, WIDTH), LAST,
                preferred_element_type=F32,
            ).astype(BF)
            for block in range(4):
                tile = result[:, block * BLOCK : (block + 1) * BLOCK]
                parts[step, block] = tile.reshape(2, HALF, BLOCK)

        @pl.when(step < UNITS)
        def _():
            for part in (0, 1):
                relay_copy(step, part).start()

        @pl.when(step == 3)
        def _():
            tok_pair(3).wait_recv()
            for part in (0, 1):
                tok_partner(3, part).start()
            up_transit.wait_recv()
            for part in (0, 1):
                up_relay(part).start()
            own_columns.start()

        @pl.when(step == PICK_STEP - 1)
        def _():
            index_z_three.wait_recv()
            to_scalars.start()

        @pl.when(step == PICK_STEP)
        def _():
            up_three.wait_recv()
            to_scalars.wait()
            own_columns.wait()
            for to_z in range(4):
                for to_x in range(4):
                    local = idx_s[to_z, to_x, 0, y] - 16 * z
                    owned = jnp.where((local >= 0) & (local < 16), 1.0, 0.0).astype(F32)
                    kept = jnp.clip(local, 0, 15)
                    factor = spread[kept // 4, kept % 4].astype(F32) * owned
                    picked[to_z, to_x] = factor.astype(BF)
            for part in (1, 0):
                up_pair(part).start()

        @pl.when(step == PAIR_STEP)
        def _():
            up_pair(1).wait_recv()
            for to_x in range(4):
                picked[3 - z, to_x] = picked[3 - z, to_x] + zpicks[1, to_x]
            up_far().start()

        @pl.when(step == FAR_STEP)
        def _():
            up_pair(0).wait_recv()
            up_far().wait_recv()
            for to_x in range(4):
                chosen[to_x] = (picked[z, to_x] + zpicks[0, to_x]) + zpicks[2, to_x]
            for n in (1, 2, 3):
                up_last(n).start()
            upfin[x] = chosen[x]

        return carry

    lax.fori_loop(0, UNITS + LAG_SUM, step_body, 0)

    def finish_sends():
        index_x_three.wait_send()
        index_z_three.wait_send()
        shrink_three.wait_send()
        up_transit.wait_send()
        remote(zpicks, zpicks, one.at[12], u2_r.at[0], partner).wait_send()
        up_last_three.wait_send()
        tok_pair(1).wait_send()

        @pl.when(core == 1)
        def _():
            tok_seconds.wait_send()
            tok_seconds_pass.wait_send()

        w_pair(2).wait_send()
        w_pair(3).wait_send()
        passed = toks.at[pl.ds(1, 2), pl.ds(0, 2)]
        remote(passed, passed, one.at[0], tokp_r.at[0], partner).wait_send()
        remote(relay, relay, one.at[1], r1_r.at[0, 0], partner).wait_send()
        remote(arrived, arrived, one.at[2], r2_r.at[0, 0], partner).wait_send()

    shrink_three.wait_recv()
    low = (shr[y] + shr_in[0] + (shr_in[1] + shr_in[2])).astype(BF)
    same = lax.broadcasted_iota(jnp.int32, (BLOCK, BLOCK), 0) == lax.broadcasted_iota(
        jnp.int32, (BLOCK, BLOCK), 1
    )
    eye = jnp.where(same, 1.0, 0.0).astype(BF)
    turned = lax.dot_general(eye, low, LAST, preferred_element_type=F32)
    doubled = (2.0 * turned).astype(BF)
    loads[5].wait()
    live = lax.broadcasted_iota(jnp.int32, (BLOCK, 1), 0) < live_ref[y]
    up_last_three.wait_recv()

    for n in (0, 2, 1, 3):
        place = (z + n) % 4
        if n:
            final_arrival(place).wait_recv()
        base = lax.dot_general(
            eye, final[place].reshape(SLICE, BLOCK), LAST, preferred_element_type=F32
        )
        extra = jnp.dot(doubled, upfin[place], preferred_element_type=F32)
        columns = pl.ds(pl.multiple_of(place * SLICE, SLICE), SLICE)
        out_ref[:, columns] = jnp.where(live, base + extra, 0.0).astype(BF)
        if n == 0:
            finish_sends()
    gone = sums.at[pl.ds(*AWAY)]
    remote(gone, gone, one.at[3], fin_r.at[z], partner).wait_send()


def body(tokens, base_up_weight, adapter_down_weight, adapter_up_weight, block_adapter_index, request_rows):
    dma = pltpu.SemaphoreType.DMA
    half_tile = (2, HALF, BLOCK)
    any_space = pl.BlockSpec(memory_space=pl.ANY)
    return pl.pallas_call(
        kernel,
        out_shape=pltpu.VMEM((BLOCK, 4 * SLICE), BF),
        in_specs=[any_space] * 6,
        out_specs=pl.BlockSpec(memory_space=pltpu.VMEM),
        scratch_shapes=[
            pltpu.VMEM((4, 4, BLOCK, WIDTH), BF),
            pltpu.VMEM((4, 2, HALF, WIDTH), BF),
            pltpu.VMEM((CATALOG, RANK, WIDTH), BF),
            pltpu.VMEM((4, RANK, 4 * SLICE), BF),
            pltpu.VMEM((UNITS, 4, *half_tile), BF),
            pltpu.VMEM((UNITS, *half_tile), BF),
            pltpu.VMEM((UNITS, 2, *half_tile), BF),
            pltpu.VMEM((UNITS, *half_tile), BF),
            pltpu.VMEM((4, 4, *half_tile), BF),
            pltpu.VMEM((4, RANK, SLICE), BF),
            pltpu.SMEM((4,), jnp.int32),
            pltpu.SMEM((4,), jnp.int32),
            pltpu.VMEM((4, 4, 1, 128), jnp.int32),
            pltpu.SMEM((4, 4, 1, 128), jnp.int32),
            pltpu.VMEM((4, 4, RANK, SLICE), BF),
            pltpu.VMEM((2, 2, RANK, SLICE), BF),
            pltpu.VMEM((4, 4, RANK, SLICE), BF),
            pltpu.VMEM((3, 4, RANK, SLICE), BF),
            pltpu.VMEM((4, RANK, SLICE), BF),
            pltpu.VMEM((4, RANK, BLOCK), F32),
            pltpu.VMEM((3, RANK, BLOCK), F32),
            dma((6,)), dma((18,)),
            dma((3,)), dma((3,)), dma((3,)), dma((3,)), dma((3,)),
            dma((4, 2)), dma((4, 2)), dma((4,)), dma((3,)),
        ],
        compiler_params=pltpu.CompilerParams(
            collective_id=0, has_side_effects=True, vmem_limit_bytes=60000000
        ),
    )(
        block_adapter_index,
        request_rows,
        tokens.reshape(4, BLOCK, WIDTH),
        base_up_weight.T.reshape(2, HALF, WIDTH),
        adapter_down_weight,
        adapter_up_weight,
    )


def solution(mesh):
    in_specs = (
        P("gx", "gy"),
        P("gy", ("gz", "gx")),
        P(None, None, "gy"),
        P("gx", None, "gz"),
        P("gx"),
        P("gx"),
    )
    out_specs = P(("gx", "gy"), "gz")
    return jax.shard_map(body, mesh=mesh, in_specs=in_specs, out_specs=out_specs, check_vma=False)
```
